256 devices in a mesh: row: 32 (over z_lo, y, core), col: 8 (over x, z_hi).
Axes of the slice: x: 4, y: 4, z: 8 (z_hi: 2, z_lo: 4; z = z_hi * 4 + z_lo), core: 2. Of those that a mesh axis runs over, the one named last changes fastest.
Arguments:
- spectral_field: float32 [2, 256, 256, 256], P(None, 'row', 'col'), may hold values from -4.5 to 4.5
Outputs:
- updated_field: float32 [2, 256, 256, 256], P(None, 'row', 'col')
- shell_spectrum: float32 [256], replicated
The draws below stay inside these ranges and needn't reach their ends.
All inputs are finite; a program needn't handle non-finite values.
Results may differ from the reference program's by a relative error of at most 0.0031.
Values may be sent and summed in bfloat16 or wider, within the bound.
A program may use at most 64 MiB of HBM per device.

```python
import math
import jax
import jax.numpy as jnp
from jax import lax

K = 256


def block_levels(key, dims, shards, smallest, top_value):
    factor_of = 1.0
    for axis_at, blocks in shards:
        draws = jax.random.uniform(jax.random.fold_in(jax.random.fold_in(key, 6), axis_at), (blocks,), jnp.float32, smallest / len(shards), top_value / len(shards))
        factor_of = factor_of * jnp.repeat(jnp.exp(draws), dims[axis_at] // blocks).reshape((-1,) + (1,) * (len(dims) - 1 - axis_at))
    return factor_of


def bell_draw(rng, shape, deviation, reach, cuts=(), kind=jnp.bfloat16):
    loudness = block_levels(rng, shape, cuts, -0.22, 0.18) if cuts else 1.0
    entries = jax.random.normal(rng, shape, jnp.float32) * deviation * loudness
    return jnp.minimum(jnp.maximum(entries, -reach), reach).astype(kind)


def setup_inputs(seed: int = 0) -> dict:
    splits = jax.random.split(jax.random.key(seed), 2)
    spectral_field = bell_draw(splits[0], (2, K, K, K), 0.7, 4.5, ((1, 32), (2, 8)), jnp.float32)
    return {"spectral_field": spectral_field}


phase_rate = 0.0002
coupling = 0.2

def wave_table(inputs, outputs, length, sine_sign, live_mask):
    phase_turns = jnp.mod(inputs[:, None] * outputs[None, :], length)
    phase_angle = phase_turns.astype(jnp.float32) * (2.0 * math.pi / length)
    live_rows = live_mask.astype(jnp.float32)[:, None]
    cosine_part = (jnp.cos(phase_angle) * live_rows).astype(jnp.bfloat16)
    sine_part = (sine_sign * jnp.sin(phase_angle) * live_rows).astype(jnp.bfloat16)
    return (cosine_part, sine_part)

def rotate(values_in, cosine_part, sine_part, einsum_form, factor):
    precise = lax.Precision.HIGHEST
    real_part = values_in[0].astype(jnp.float32)
    imag_part = values_in[1].astype(jnp.float32)
    cos_wide = cosine_part.astype(jnp.float32)
    sin_wide = sine_part.astype(jnp.float32)
    out_real = jnp.einsum(einsum_form, real_part, cos_wide, precision=precise) - jnp.einsum(einsum_form, imag_part, sin_wide, precision=precise)
    out_imag = jnp.einsum(einsum_form, real_part, sin_wide, precision=precise) + jnp.einsum(einsum_form, imag_part, cos_wide, precision=precise)
    return jnp.stack([out_real, out_imag]) * factor

def reference(spectral_field):
    mode_count = spectral_field.shape[1]
    grid_count = 2 * mode_count
    wavenumbers = jnp.arange(mode_count, dtype=jnp.int32) - mode_count // 2
    grid_points = jnp.arange(grid_count, dtype=jnp.int32)
    inv_cos, inv_sin = wave_table(wavenumbers, grid_points, grid_count, 1.0, jnp.ones((mode_count,), bool))
    fwd_cos, fwd_sin = wave_table(grid_points, wavenumbers, grid_count, -1.0, jnp.ones((grid_count,), bool))
    scale_in = 1.0 / math.sqrt(mode_count)
    scale_out = math.sqrt(mode_count) / grid_count
    coeffs = spectral_field.astype(jnp.bfloat16)
    along_z = rotate(coeffs, inv_cos, inv_sin, 'abc,cd->abd', scale_in).astype(jnp.bfloat16)
    along_y = rotate(along_z, inv_cos, inv_sin, 'abc,bd->adc', scale_in).astype(jnp.bfloat16)
    block_size = grid_count // 8
    pieces = []
    for number in range(8):
        z_block = lax.slice_in_dim(along_y, number * block_size, (number + 1) * block_size, axis=3)
        physical = rotate(z_block, inv_cos, inv_sin, 'abc,ad->dbc', scale_in)
        cubic_term = (coupling * (physical[0] * physical[0] + physical[1] * physical[1]) * physical).astype(jnp.bfloat16)
        pieces.append(rotate(cubic_term, fwd_cos, fwd_sin, 'abc,ad->dbc', scale_out).astype(jnp.bfloat16))
    back_x = jnp.concatenate(pieces, axis=3)
    back_y = rotate(back_x, fwd_cos, fwd_sin, 'abc,bd->adc', scale_out).astype(jnp.bfloat16)
    nonlinear = rotate(back_y, fwd_cos, fwd_sin, 'abc,cd->abd', scale_out)
    wave_first = wavenumbers[:, None, None]
    wave_second = wavenumbers[None, :, None]
    wave_third = wavenumbers[None, None, :]
    squared = wave_first * wave_first + wave_second * wave_second + wave_third * wave_third
    phase_angle = phase_rate * squared.astype(jnp.float32)
    cosine_part = jnp.cos(phase_angle)
    sine_part = jnp.sin(phase_angle)
    shifted_real = spectral_field[0] - nonlinear[1]
    shifted_imag = spectral_field[1] + nonlinear[0]
    new_real = shifted_real * cosine_part + shifted_imag * sine_part
    new_imag = shifted_imag * cosine_part - shifted_real * sine_part
    updated_field = jnp.stack([new_real, new_imag])
    energy = new_real * new_real + new_imag * new_imag
    shell_index = jnp.floor(jnp.sqrt(squared.astype(jnp.float32)) + 0.5).astype(jnp.int32)
    totals = jax.ops.segment_sum(energy.reshape(-1), shell_index.reshape(-1), num_segments=mode_count)
    counts = jax.ops.segment_sum(jnp.ones_like(energy).reshape(-1), shell_index.reshape(-1), num_segments=mode_count)
    shell_spectrum = totals / jnp.maximum(counts, 1.0)
    return (updated_field, shell_spectrum)
```

```python
import functools
import math

import jax
import jax.numpy as jnp
import numpy as np
from jax import lax
from jax.experimental import pallas as pl
from jax.experimental.pallas import tpu as pltpu
from jax.sharding import PartitionSpec as P

PHASE_RATE = 0.0002
COUPLING = 0.2
K = 256
N = 512
BF16 = jnp.bfloat16
F32 = jnp.float32


def mm(a, b):
    return lax.dot_general(a, b, (((1,), (0,)), ((), ())), preferred_element_type=F32)


def mmt(a, b):
    return lax.dot_general(a, b, (((1,), (1,)), ((), ())), preferred_element_type=F32)


def iota(shape, dim):
    return lax.broadcasted_iota(jnp.int32, shape, dim)


def one_hot(hit):
    return jnp.where(hit, 1.0, 0.0).astype(BF16)


def transform_kernel(
    field, fwd, inv, out,
    p1, p2, p3, aout, bin_, yb, bout, cin, dz, cub, cout, din, dout, ein, zb,
    s1, r1, s2, r2, s3, r3, s4, r4,
):
    row = lax.axis_index("row")
    xh = lax.axis_index("col")
    zl = row // 8
    yc = row % 8

    def remote(src, dst, send, recv, to_row, to_col):
        return pltpu.make_async_remote_copy(
            src_ref=src, dst_ref=dst, send_sem=send, recv_sem=recv,
            device_id={"row": to_row, "col": to_col}, device_id_type=pl.DeviceIdType.MESH,
        )

    barrier = pltpu.get_barrier_semaphore()

    @pl.loop(1, 32)
    def _(i):
        d = (zl * 8 + xh + i) % 32
        pl.semaphore_signal(
            barrier, inc=1, device_id={"row": (d // 8) * 8 + yc, "col": d % 8},
            device_id_type=pl.DeviceIdType.MESH,
        )

    @pl.loop(1, 8)
    def _(j):
        pl.semaphore_signal(
            barrier, inc=1, device_id={"row": zl * 8 + (yc + j) % 8, "col": xh},
            device_id_type=pl.DeviceIdType.MESH,
        )

    def copy1(k, i):
        zd = (zl + 4 - k) % 4
        xd = (xh + i) % 8
        return remote(aout.at[zd, xd], bin_.at[zl, xh], s1.at[k, i], r1.at[k, i], zd * 8 + yc, xd)

    def copy2(k, j):
        zs = (zl + k) % 4
        yd = (yc + j) % 8
        return remote(bout.at[yd, :, zs], cin.at[yc, :, zs], s2.at[k, j], r2.at[k, j], zl * 8 + yd, xh)

    def copy3(k, j):
        zs = (zl + k) % 4
        yd = (yc + j) % 8
        return remote(cout.at[yd, zs], din.at[yc, zs], s3.at[k, j], r3.at[k, j], zl * 8 + yd, xh)

    def copy4(k, i):
        zd = (zl + k) % 4
        xd = (xh + i) % 8
        return remote(dout.at[zd, xd], ein.at[zl, xh], s4.at[k, i], r4.at[k, i], zd * 8 + yc, xd)

    def stage_a(k):
        zd = (zl + 4 - k) % 4
        rows = pl.ds(pl.multiple_of(zd * 128, 128), 128)
        c, s = inv[rows, :256], inv[rows, 256:]
        re = field[0].reshape(256, 256).astype(BF16)
        im = field[1].reshape(256, 256).astype(BF16)
        out_re = (mmt(c, re) - mmt(s, im)) * (1.0 / 16.0)
        out_im = (mmt(s, re) + mmt(c, im)) * (1.0 / 16.0)
        aout[zd, :, 0] = out_re.astype(BF16).reshape(8, 16, 256)
        aout[zd, :, 1] = out_im.astype(BF16).reshape(8, 16, 256)

    @pl.loop(0, 4)
    def _(k):
        stage_a(k)

    bin_[zl, xh] = aout[zl, xh]
    pl.semaphore_wait(barrier, 38)

    @pl.loop(1, 8)
    def _(i):
        copy1(0, i).start()

    @pl.loop(1, 4)
    def _(k):
        @pl.loop(0, 8)
        def _(i):
            copy1(k, i).start()

    j1 = iota((128, 512), 1)
    f1 = ((j1 // 32) % 4) * 128 + (j1 // 128) * 32 + j1 % 32

    @pl.loop(0, 4)
    def _(b):
        rows = pl.ds(pl.multiple_of(b * 128, 128), 128)
        p1[rows, :] = one_hot(iota((128, 512), 0) + b * 128 == f1)

    q2 = iota((256, 256), 0)
    p2[...] = one_hot(iota((256, 256), 1) == (q2 % 32) * 8 + q2 // 32)

    j3 = iota((128, 1024), 1)
    f3 = ((j3 // 16) % 8) * 128 + (j3 % 16) * 8 + j3 // 128

    @pl.loop(0, 8)
    def _(b):
        rows = pl.ds(pl.multiple_of(b * 128, 128), 128)
        p3[rows, :] = one_hot(iota((128, 1024), 0) + b * 128 == f3)

    def stage_b(k):
        zs = (zl + k) % 4
        parts = []
        for ht in range(2):
            for xt in range(2):
                lanes = slice(xt * 128, xt * 128 + 128)
                parts.append(jnp.concatenate(
                    [bin_[zs, ht * 4 + h, :, :, lanes].reshape(32, 128) for h in range(4)], axis=1))
        o = mm(jnp.concatenate(parts, axis=0), p1[...]).astype(BF16)
        for ht in range(2):
            for xt in range(2):
                base = (ht * 2 + xt) * 32
                for c in range(2):
                    for x in range(4):
                        yb[c, xt * 4 + x, :, ht * 128:ht * 128 + 128] = (
                            o[base + c * 16:base + c * 16 + 16, x * 128:x * 128 + 128])
        re = yb[0].reshape(128, 256)
        im = yb[1].reshape(128, 256)
        cos, sin = fwd[:256, :], fwd[256:, :]
        for c in range(2):
            if c == 0:
                v = (mm(re, cos) - mm(im, sin)) * (1.0 / 16.0)
            else:
                v = (mm(re, sin) + mm(im, cos)) * (1.0 / 16.0)
            for y in range(4):
                w = v[:, y * 128:y * 128 + 128].reshape(8, 2, 8, 128)
                for zh in range(2):
                    bout[y * 2 + zh, c, zs] = w[:, zh].astype(BF16)

    @pl.loop(0, 4)
    def _(k):
        @pl.when(k > 0)
        def _():
            copy1(k, 0).wait_recv()

        @pl.loop(1, 8)
        def _(i):
            copy1(k, i).wait_recv()

        stage_b(k)

        @pl.loop(1, 8)
        def _(j):
            copy2(k, j).start()

    cin[yc] = bout[yc]

    @pl.loop(0, 4)
    def _(k):
        @pl.loop(1, 8)
        def _(j):
            copy2(k, j).wait_recv()

    @pl.loop(0, 8)
    def _(s):
        d = jnp.concatenate([cin[s, 0].reshape(256, 128), cin[s, 1].reshape(256, 128)], axis=1)
        dz[:, :, s] = mm(p2[...], d).reshape(8, 4, 8, 256).astype(BF16)

    @pl.loop(0, 8)
    def _(z):
        d = dz[z].reshape(256, 256)
        d2 = jnp.concatenate([-d[:, 128:], d[:, :128]], axis=1)
        for h in range(4):
            rows = slice(h * 128, h * 128 + 128)
            phys = (mm(inv[rows, :256], d) + mm(inv[rows, 256:], d2)) * (1.0 / 16.0)
            re, im = phys[:, :128], phys[:, 128:]
            gain = COUPLING * (re * re + im * im)
            cub[rows, :128] = (gain * re).astype(BF16)
            cub[rows, 128:] = (gain * im).astype(BF16)
        m1 = mm(fwd[:256, :], cub[...])
        m2 = mm(fwd[256:, :], cub[...])
        back = ((m1[:, :128] + m2[:, 128:]) * (1.0 / 32.0), (m1[:, 128:] - m2[:, :128]) * (1.0 / 32.0))
        for c in range(2):
            v = back[c].reshape(4, 8, 8, 128)
            for q in range(4):
                cout[:, q, z, c] = v[q].astype(BF16)

    @pl.loop(0, 4)
    def _(k):
        @pl.loop(1, 8)
        def _(j):
            copy3(k, j).start()

    din[yc] = cout[yc]

    def stage_d(k):
        zs = (zl + k) % 4
        r = []
        for c in range(2):
            r.append(jnp.concatenate([
                jnp.concatenate([din[y * 2 + zh, zs, :, c].reshape(64, 128) for zh in range(2)], axis=0)
                for y in range(4)], axis=1))
        r = jnp.concatenate(r, axis=0)
        o1 = mmt(fwd[:256, :], r)
        o2 = mmt(fwd[256:, :], r)
        re = (o1[:, :128] + o2[:, 128:]) * (1.0 / 32.0)
        im = (o1[:, 128:] - o2[:, :128]) * (1.0 / 32.0)
        dout[zs, :, 0] = re.astype(BF16).reshape(8, 32, 128)
        dout[zs, :, 1] = im.astype(BF16).reshape(8, 32, 128)

    @pl.loop(0, 4)
    def _(k):
        @pl.loop(1, 8)
        def _(j):
            copy3(k, j).wait_recv()

        stage_d(k)

        @pl.when(k > 0)
        def _():
            copy4(k, 0).start()

        @pl.loop(1, 8)
        def _(i):
            copy4(k, i).start()

    ein[zl, xh] = dout[zl, xh]

    @pl.loop(0, 4)
    def _(k):
        @pl.when(k > 0)
        def _():
            copy4(k, 0).wait_recv()

        @pl.loop(1, 8)
        def _(i):
            copy4(k, i).wait_recv()

    for g in range(4):
        o = mm(jnp.concatenate([ein[g, s].reshape(64, 128) for s in range(8)], axis=1), p3[...]).astype(BF16)
        for c in range(2):
            for x in range(8):
                zb[c, x, :, g * 128:g * 128 + 128] = o[c * 32:c * 32 + 32, x * 128:x * 128 + 128]
    re = zb[0].reshape(256, 512)
    im = zb[1].reshape(256, 512)
    cos, sin = inv[:, :256], inv[:, 256:]
    out[0] = (mm(re, cos) + mm(im, sin)) * (1.0 / 32.0)
    out[1] = (mm(im, cos) - mm(re, sin)) * (1.0 / 32.0)

    @pl.loop(0, 4)
    def _(k):
        @pl.when(k > 0)
        def _():
            copy1(k, 0).wait_send()
            copy4(k, 0).wait_send()

        @pl.loop(1, 8)
        def _(i):
            copy1(k, i).wait_send()
            copy2(k, i).wait_send()
            copy3(k, i).wait_send()
            copy4(k, i).wait_send()


def update_kernel(field, nonlinear, updated, shells):
    wx0 = lax.axis_index("row") * 8 - 128
    wy0 = lax.axis_index("col") * 32 - 128
    wz = iota((1, 256), 1) - 128
    az = PHASE_RATE * (wz * wz).astype(F32)
    cz, sz = jnp.cos(az), jnp.sin(az)
    r = iota((256, 1), 0)
    wx = wx0 + r // 32
    wy = wy0 + r % 32
    r2 = wx * wx + wy * wy
    ar = PHASE_RATE * r2.astype(F32)
    cr, sr = jnp.cos(ar), jnp.sin(ar)
    cos = cr * cz - sr * sz
    sin = sr * cz + cr * sz
    u = field[0] - nonlinear[1]
    v = field[1] + nonlinear[0]
    re = u * cos + v * sin
    im = v * cos - u * sin
    updated[0] = re
    updated[1] = im
    energy = re * re + im * im
    j = jnp.abs(iota((256, 128), 0) - 128)
    within = jnp.where(j <= iota((256, 128), 1), 1.0, 0.0)
    prefix = lax.dot_general(energy, within, (((1,), (0,)), ((), ())),
                             preferred_element_type=F32, precision=lax.Precision.HIGHEST)
    parts = []
    for t in range(2):
        s = iota((1, 128), 1) + t * 128
        room = s * s + s - r2
        m = jnp.sqrt(jnp.maximum(room, 0).astype(F32) + 0.5).astype(jnp.int32)
        inner = jnp.take_along_axis(prefix, jnp.minimum(m, 127), axis=1, mode="promise_in_bounds")
        total = jnp.where(room >= 0, inner, 0.0) + jnp.where(room >= 128 * 128, energy[:, :1], 0.0)
        parts.append(jnp.sum(total, axis=0, keepdims=True))
    full = jnp.concatenate(parts, axis=1)
    lane = iota((1, 256), 1)
    shifted = jnp.concatenate([pltpu.roll(parts[0], 1, 1), pltpu.roll(parts[1], 1, 1)], axis=1)
    shifted = jnp.where(lane == 0, 0.0, jnp.where(lane == 128, parts[0][:, 127:], shifted))
    shells[...] = full - shifted


def reduce_kernel(shells, counts, out, first, second, mid, s1, r1, s2, r2):
    row = lax.axis_index("row")
    xh = lax.axis_index("col")
    zl = row // 8
    yc = row % 8
    me = zl * 8 + xh

    def copy1(i):
        d = (me + i) % 32
        return pltpu.make_async_remote_copy(
            src_ref=shells, dst_ref=first.at[me], send_sem=s1.at[i], recv_sem=r1.at[i],
            device_id={"row": (d // 8) * 8 + yc, "col": d % 8}, device_id_type=pl.DeviceIdType.MESH)

    def copy2(j):
        return pltpu.make_async_remote_copy(
            src_ref=mid, dst_ref=second.at[yc], send_sem=s2.at[j], recv_sem=r2.at[j],
            device_id={"row": zl * 8 + (yc + j) % 8, "col": xh}, device_id_type=pl.DeviceIdType.MESH)

    barrier = pltpu.get_barrier_semaphore()

    @pl.loop(1, 32)
    def _(i):
        d = (me + i) % 32
        pl.semaphore_signal(
            barrier, inc=1, device_id={"row": (d // 8) * 8 + yc, "col": d % 8},
            device_id_type=pl.DeviceIdType.MESH)

    @pl.loop(1, 8)
    def _(j):
        pl.semaphore_signal(
            barrier, inc=1, device_id={"row": zl * 8 + (yc + j) % 8, "col": xh},
            device_id_type=pl.DeviceIdType.MESH)

    first[me] = shells[...]
    pl.semaphore_wait(barrier, 38)

    @pl.loop(1, 32)
    def _(i):
        copy1(i).start()

    @pl.loop(1, 32)
    def _(i):
        copy1(i).wait_recv()

    mid[...] = jnp.sum(first[...], axis=0)
    second[yc] = mid[...]

    @pl.loop(1, 8)
    def _(j):
        copy2(j).start()

    @pl.loop(1, 8)
    def _(j):
        copy2(j).wait_recv()

    out[...] = jnp.sum(second[...], axis=0) / counts[...]

    @pl.loop(1, 32)
    def _(i):
        copy1(i).wait_send()

    @pl.loop(1, 8)
    def _(j):
        copy2(j).wait_send()


def tables():
    waves = np.arange(K, dtype=np.int64) - K // 2
    phase = (waves[:, None] * np.arange(N, dtype=np.int64)[None, :]) % N
    angle = phase.astype(np.float32) * np.float32(2.0 * math.pi / N)
    cos = np.cos(angle).astype(jnp.bfloat16)
    sin = np.sin(angle).astype(jnp.bfloat16)
    fwd = np.concatenate([cos, sin], axis=0)
    inv = np.concatenate([cos.T, sin.T], axis=1)
    sq = waves * waves
    q = (sq[:, None] + sq[None, :]).reshape(-1)
    pairs = np.bincount(q, minlength=2 * (K // 2) ** 2 + 1)
    counts = np.zeros(K, np.float64)
    radii = np.nonzero(pairs)[0]
    for w2 in sq:
        shell = np.floor(np.sqrt((radii + w2).astype(np.float64)) + 0.5).astype(np.int64)
        counts += np.bincount(shell, weights=pairs[radii], minlength=K)[:K]
    return fwd, np.ascontiguousarray(inv), np.maximum(counts, 1.0).astype(np.float32).reshape(1, K)


VMEM = pl.BlockSpec(memory_space=pltpu.VMEM)


def body(spectral_field, fwd, inv, counts):
    nonlinear = pl.pallas_call(
        transform_kernel,
        out_shape=jax.ShapeDtypeStruct((2, 256, 256), F32),
        in_specs=[VMEM] * 3,
        out_specs=VMEM,
        scratch_shapes=[
            pltpu.VMEM((512, 512), BF16),
            pltpu.VMEM((256, 256), BF16),
            pltpu.VMEM((1024, 1024), BF16),
            pltpu.VMEM((4, 8, 2, 16, 256), BF16),
            pltpu.VMEM((4, 8, 2, 16, 256), BF16),
            pltpu.VMEM((2, 8, 16, 256), BF16),
            pltpu.VMEM((8, 2, 4, 8, 8, 128), BF16),
            pltpu.VMEM((8, 2, 4, 8, 8, 128), BF16),
            pltpu.VMEM((8, 4, 8, 8, 256), BF16),
            pltpu.VMEM((512, 256), BF16),
            pltpu.VMEM((8, 4, 8, 2, 8, 128), BF16),
            pltpu.VMEM((8, 4, 8, 2, 8, 128), BF16),
            pltpu.VMEM((4, 8, 2, 32, 128), BF16),
            pltpu.VMEM((4, 8, 2, 32, 128), BF16),
            pltpu.VMEM((2, 8, 32, 512), BF16),
        ] + [pltpu.SemaphoreType.DMA((4, 8))] * 8,
        compiler_params=pltpu.CompilerParams(
            collective_id=0, has_side_effects=True, vmem_limit_bytes=48 * 1024 * 1024),
        name="transforms",
    )(spectral_field, fwd, inv)

    updated, shells = pl.pallas_call(
        update_kernel,
        out_shape=(jax.ShapeDtypeStruct((2, 256, 256), F32), jax.ShapeDtypeStruct((1, 256), F32)),
        in_specs=[VMEM] * 2,
        out_specs=(VMEM, VMEM),
        name="update",
    )(spectral_field.reshape(2, 256, 256), nonlinear)

    spectrum = pl.pallas_call(
        reduce_kernel,
        out_shape=jax.ShapeDtypeStruct((1, 256), F32),
        in_specs=[VMEM] * 2,
        out_specs=VMEM,
        scratch_shapes=[
            pltpu.VMEM((32, 1, 256), F32),
            pltpu.VMEM((8, 1, 256), F32),
            pltpu.VMEM((1, 256), F32),
            pltpu.SemaphoreType.DMA((32,)),
            pltpu.SemaphoreType.DMA((32,)),
            pltpu.SemaphoreType.DMA((8,)),
            pltpu.SemaphoreType.DMA((8,)),
        ],
        compiler_params=pltpu.CompilerParams(collective_id=1, has_side_effects=True),
        name="reduce",
    )(shells, counts)
    return updated.reshape(2, 8, 32, 256), spectrum.reshape(256)


def solution(mesh):
    fwd, inv, counts = tables()
    step = functools.partial(jax.shard_map, mesh=mesh, check_vma=False)

    def run(spectral_field):
        return step(
            lambda f: body(f, jnp.asarray(fwd), jnp.asarray(inv), jnp.asarray(counts)),
            in_specs=(P(None, "row", "col", None),),
            out_specs=(P(None, "row", "col", None), P()),
        )(spectral_field)

    return run
```

```python
import functools
import math

import jax
import jax.numpy as jnp
import numpy as np
from jax import lax
from jax.experimental import pallas as pl
from jax.experimental.pallas import tpu as pltpu
from jax.sharding import PartitionSpec as P

PHASE_RATE = 0.0002
COUPLING = 0.2
K = 256
N = 512
BF16 = jnp.bfloat16
F32 = jnp.float32


def mm(a, b):
    return lax.dot_general(a, b, (((1,), (0,)), ((), ())), preferred_element_type=F32)


def mmt(a, b):
    return lax.dot_general(a, b, (((1,), (1,)), ((), ())), preferred_element_type=F32)


def iota(shape, dim):
    return lax.broadcasted_iota(jnp.int32, shape, dim)


def one_hot(hit):
    return jnp.where(hit, 1.0, 0.0).astype(BF16)


def shell_sums(energy, r2):
    j = jnp.abs(iota((256, 128), 0) - 128)
    within = jnp.where(j <= iota((256, 128), 1), 1.0, 0.0)
    prefix = lax.dot_general(energy, within, (((1,), (0,)), ((), ())),
                             preferred_element_type=F32, precision=lax.Precision.HIGHEST)
    parts = []
    for t in range(2):
        s = iota((1, 128), 1) + t * 128
        room = s * s + s - r2
        m = jnp.sqrt(jnp.maximum(room, 0).astype(F32) + 0.5).astype(jnp.int32)
        inner = jnp.take_along_axis(prefix, jnp.minimum(m, 127), axis=1, mode="promise_in_bounds")
        total = jnp.where(room >= 0, inner, 0.0) + jnp.where(room >= 128 * 128, energy[:, :1], 0.0)
        parts.append(jnp.sum(total, axis=0, keepdims=True))
    lane = iota((1, 256), 1)
    shifted = jnp.concatenate([pltpu.roll(parts[0], 1, 1), pltpu.roll(parts[1], 1, 1)], axis=1)
    shifted = jnp.where(lane == 0, 0.0, jnp.where(lane == 128, parts[0][:, 127:], shifted))
    return jnp.concatenate(parts, axis=1) - shifted


def transform_kernel(
    field_hbm, fwd_hbm, inv_hbm, counts, out, spectrum,
    field, fwd, inv, p1, p2, p3, aout, bin_, yb, bout, cin, dz, cub, cout, din, dout, ein, zb,
    shells, first, second, mid,
    s1, r1, s2, r2, s3, r3, s4, r4, load_sem, s5, r5, s6, r6,
):
    row = lax.axis_index("row")
    xh = lax.axis_index("col")
    zl = row // 8
    yc = row % 8

    def remote(src, dst, send, recv, to_row, to_col):
        return pltpu.make_async_remote_copy(
            src_ref=src, dst_ref=dst, send_sem=send, recv_sem=recv,
            device_id={"row": to_row, "col": to_col}, device_id_type=pl.DeviceIdType.MESH,
        )

    loads = [
        pltpu.make_async_copy(field_hbm, field, load_sem.at[0]),
        pltpu.make_async_copy(inv_hbm, inv, load_sem.at[1]),
        pltpu.make_async_copy(fwd_hbm, fwd, load_sem.at[2]),
    ]
    for load in loads:
        load.start()

    barrier = pltpu.get_barrier_semaphore()

    @pl.loop(1, 32)
    def _(i):
        d = (zl * 8 + xh + i) % 32
        pl.semaphore_signal(
            barrier, inc=1, device_id={"row": (d // 8) * 8 + yc, "col": d % 8},
            device_id_type=pl.DeviceIdType.MESH,
        )

    @pl.loop(1, 8)
    def _(j):
        pl.semaphore_signal(
            barrier, inc=1, device_id={"row": zl * 8 + (yc + j) % 8, "col": xh},
            device_id_type=pl.DeviceIdType.MESH,
        )

    def copy1(k, i):
        zd = (zl + 4 - k) % 4
        xd = (xh + i) % 8
        return remote(aout.at[zd, xd], bin_.at[zl, xh], s1.at[k, i], r1.at[k, i], zd * 8 + yc, xd)

    def copy2(k, j):
        zs = (zl + k) % 4
        yd = (yc + j) % 8
        return remote(bout.at[yd, :, zs], cin.at[yc, :, zs], s2.at[k, j], r2.at[k, j], zl * 8 + yd, xh)

    def copy3(k, j):
        zs = (zl + k) % 4
        yd = (yc + j) % 8
        return remote(cout.at[yd, zs], din.at[yc, zs], s3.at[k, j], r3.at[k, j], zl * 8 + yd, xh)

    def copy4(k, i):
        zd = (zl + k) % 4
        xd = (xh + i) % 8
        return remote(dout.at[zd, xd], ein.at[zl, xh], s4.at[k, i], r4.at[k, i], zd * 8 + yc, xd)

    me1 = zl * 8 + xh

    def copy5(i):
        d = (me1 + i) % 32
        return remote(shells, first.at[me1], s5.at[i], r5.at[i], (d // 8) * 8 + yc, d % 8)

    def copy6(j):
        return remote(mid, second.at[yc], s6.at[j], r6.at[j], zl * 8 + (yc + j) % 8, xh)

    j1 = iota((128, 512), 1)
    f1 = ((j1 // 32) % 4) * 128 + (j1 // 128) * 32 + j1 % 32

    @pl.loop(0, 4)
    def _(b):
        rows = pl.ds(pl.multiple_of(b * 128, 128), 128)
        p1[rows, :] = one_hot(iota((128, 512), 0) + b * 128 == f1)

    q2 = iota((256, 256), 0)
    p2[...] = one_hot(iota((256, 256), 1) == (q2 % 32) * 8 + q2 // 32)

    j3 = iota((128, 1024), 1)
    f3 = ((j3 // 16) % 8) * 128 + (j3 % 16) * 8 + j3 // 128

    @pl.loop(0, 8)
    def _(b):
        rows = pl.ds(pl.multiple_of(b * 128, 128), 128)
        p3[rows, :] = one_hot(iota((128, 1024), 0) + b * 128 == f3)

    def stage_a(k):
        zd = (zl + 4 - k) % 4
        rows = pl.ds(pl.multiple_of(zd * 128, 128), 128)
        c, s = inv[rows, :256], inv[rows, 256:]
        re = field[0].reshape(256, 256).astype(BF16)
        im = field[1].reshape(256, 256).astype(BF16)
        out_re = (mmt(c, re) - mmt(s, im)) * (1.0 / 16.0)
        out_im = (mmt(s, re) + mmt(c, im)) * (1.0 / 16.0)
        aout[zd, :, 0] = out_re.astype(BF16).reshape(8, 16, 256)
        aout[zd, :, 1] = out_im.astype(BF16).reshape(8, 16, 256)

    loads[0].wait()
    loads[1].wait()

    @pl.loop(0, 4)
    def _(k):
        stage_a(k)

    bin_[zl, xh] = aout[zl, xh]
    pl.semaphore_wait(barrier, 38)

    @pl.loop(1, 8)
    def _(i):
        copy1(0, i).start()

    @pl.loop(1, 4)
    def _(k):
        @pl.loop(0, 8)
        def _(i):
            copy1(k, i).start()

    def stage_b(k):
        zs = (zl + k) % 4
        parts = []
        for ht in range(2):
            for xt in range(2):
                lanes = slice(xt * 128, xt * 128 + 128)
                parts.append(jnp.concatenate(
                    [bin_[zs, ht * 4 + h, :, :, lanes].reshape(32, 128) for h in range(4)], axis=1))
        o = mm(jnp.concatenate(parts, axis=0), p1[...]).astype(BF16)
        for ht in range(2):
            for xt in range(2):
                base = (ht * 2 + xt) * 32
                for c in range(2):
                    for x in range(4):
                        yb[c, xt * 4 + x, :, ht * 128:ht * 128 + 128] = (
                            o[base + c * 16:base + c * 16 + 16, x * 128:x * 128 + 128])
        re = yb[0].reshape(128, 256)
        im = yb[1].reshape(128, 256)
        cos, sin = fwd[:256, :], fwd[256:, :]
        for c in range(2):
            if c == 0:
                v = (mm(re, cos) - mm(im, sin)) * (1.0 / 16.0)
            else:
                v = (mm(re, sin) + mm(im, cos)) * (1.0 / 16.0)
            for y in range(4):
                w = v[:, y * 128:y * 128 + 128].reshape(8, 2, 8, 128)
                for zh in range(2):
                    bout[y * 2 + zh, c, zs] = w[:, zh].astype(BF16)

    loads[2].wait()

    @pl.loop(0, 4)
    def _(k):
        @pl.when(k > 0)
        def _():
            copy1(k, 0).wait_recv()

        @pl.loop(1, 8)
        def _(i):
            copy1(k, i).wait_recv()

        stage_b(k)

        @pl.loop(1, 8)
        def _(j):
            copy2(k, j).start()

    cin[yc] = bout[yc]

    @pl.loop(0, 4)
    def _(k):
        @pl.loop(1, 8)
        def _(j):
            copy2(k, j).wait_recv()

    @pl.loop(0, 8)
    def _(s):
        d = jnp.concatenate([cin[s, 0].reshape(256, 128), cin[s, 1].reshape(256, 128)], axis=1)
        dz[:, :, s] = mm(p2[...], d).reshape(8, 4, 8, 256).astype(BF16)

    @pl.loop(0, 8)
    def _(z):
        d = dz[z].reshape(256, 256)
        d2 = jnp.concatenate([-d[:, 128:], d[:, :128]], axis=1)
        for h in range(4):
            rows = slice(h * 128, h * 128 + 128)
            phys = (mm(inv[rows, :256], d) + mm(inv[rows, 256:], d2)) * (1.0 / 16.0)
            re, im = phys[:, :128], phys[:, 128:]
            gain = COUPLING * (re * re + im * im)
            cub[rows, :128] = (gain * re).astype(BF16)
            cub[rows, 128:] = (gain * im).astype(BF16)
        m1 = mm(fwd[:256, :], cub[...])
        m2 = mm(fwd[256:, :], cub[...])
        back = ((m1[:, :128] + m2[:, 128:]) * (1.0 / 32.0), (m1[:, 128:] - m2[:, :128]) * (1.0 / 32.0))
        for c in range(2):
            v = back[c].reshape(4, 8, 8, 128)
            for q in range(4):
                cout[:, q, z, c] = v[q].astype(BF16)

    @pl.loop(0, 4)
    def _(k):
        @pl.loop(1, 8)
        def _(j):
            copy3(k, j).start()

    din[yc] = cout[yc]

    def stage_d(k):
        zs = (zl + k) % 4
        r = []
        for c in range(2):
            r.append(jnp.concatenate([
                jnp.concatenate([din[y * 2 + zh, zs, :, c].reshape(64, 128) for zh in range(2)], axis=0)
                for y in range(4)], axis=1))
        r = jnp.concatenate(r, axis=0)
        o1 = mmt(fwd[:256, :], r)
        o2 = mmt(fwd[256:, :], r)
        re = (o1[:, :128] + o2[:, 128:]) * (1.0 / 32.0)
        im = (o1[:, 128:] - o2[:, :128]) * (1.0 / 32.0)
        dout[zs, :, 0] = re.astype(BF16).reshape(8, 32, 128)
        dout[zs, :, 1] = im.astype(BF16).reshape(8, 32, 128)

    @pl.loop(0, 4)
    def _(k):
        @pl.loop(1, 8)
        def _(j):
            copy3(k, j).wait_recv()

        stage_d(k)

        @pl.when(k > 0)
        def _():
            copy4(k, 0).start()

        @pl.loop(1, 8)
        def _(i):
            copy4(k, i).start()

    ein[zl, xh] = dout[zl, xh]

    @pl.loop(0, 4)
    def _(k):
        @pl.when(k > 0)
        def _():
            copy4(k, 0).wait_recv()

        @pl.loop(1, 8)
        def _(i):
            copy4(k, i).wait_recv()

    for g in range(4):
        o = mm(jnp.concatenate([ein[g, s].reshape(64, 128) for s in range(8)], axis=1), p3[...]).astype(BF16)
        for c in range(2):
            for x in range(8):
                zb[c, x, :, g * 128:g * 128 + 128] = o[c * 32:c * 32 + 32, x * 128:x * 128 + 128]
    re = zb[0].reshape(256, 512)
    im = zb[1].reshape(256, 512)
    cos, sin = inv[:, :256], inv[:, 256:]
    nl_re = (mm(re, cos) + mm(im, sin)) * (1.0 / 32.0)
    nl_im = (mm(im, cos) - mm(re, sin)) * (1.0 / 32.0)
    u = field[0].reshape(256, 256) - nl_im
    v = field[1].reshape(256, 256) + nl_re
    out[0] = u.reshape(8, 32, 256)
    out[1] = v.reshape(8, 32, 256)

    wz = iota((1, 256), 1) - 128
    r = iota((256, 1), 0)
    wx = row * 8 - 128 + r // 32
    wy = xh * 32 - 128 + r % 32
    rad2 = wx * wx + wy * wy
    shells[...] = shell_sums(u * u + v * v, rad2)
    first[me1] = shells[...]

    @pl.loop(1, 32)
    def _(i):
        copy5(i).start()

    az = PHASE_RATE * (wz * wz).astype(F32)
    ar = PHASE_RATE * rad2.astype(F32)
    cz, sz = jnp.cos(az), jnp.sin(az)
    cr, sr = jnp.cos(ar), jnp.sin(ar)
    cos = (cr * cz - sr * sz).reshape(8, 32, 256)
    sin = (sr * cz + cr * sz).reshape(8, 32, 256)
    u, v = out[0], out[1]
    out[0] = u * cos + v * sin
    out[1] = v * cos - u * sin

    @pl.loop(1, 32)
    def _(i):
        copy5(i).wait_recv()

    mid[...] = jnp.sum(first[...], axis=0)
    second[yc] = mid[...]

    @pl.loop(1, 8)
    def _(j):
        copy6(j).start()

    @pl.loop(1, 8)
    def _(j):
        copy6(j).wait_recv()

    spectrum[...] = jnp.sum(second[...], axis=0) / counts[...]

    @pl.loop(0, 4)
    def _(k):
        @pl.when(k > 0)
        def _():
            copy1(k, 0).wait_send()
            copy4(k, 0).wait_send()

        @pl.loop(1, 8)
        def _(i):
            copy1(k, i).wait_send()
            copy2(k, i).wait_send()
            copy3(k, i).wait_send()
            copy4(k, i).wait_send()

    @pl.loop(1, 32)
    def _(i):
        copy5(i).wait_send()

    @pl.loop(1, 8)
    def _(j):
        copy6(j).wait_send()


def tables():
    waves = np.arange(K, dtype=np.int64) - K // 2
    phase = (waves[:, None] * np.arange(N, dtype=np.int64)[None, :]) % N
    angle = phase.astype(np.float32) * np.float32(2.0 * math.pi / N)
    cos = np.cos(angle).astype(jnp.bfloat16)
    sin = np.sin(angle).astype(jnp.bfloat16)
    fwd = np.concatenate([cos, sin], axis=0)
    inv = np.concatenate([cos.T, sin.T], axis=1)
    sq = waves * waves
    q = (sq[:, None] + sq[None, :]).reshape(-1)
    pairs = np.bincount(q, minlength=2 * (K // 2) ** 2 + 1)
    counts = np.zeros(K, np.float64)
    radii = np.nonzero(pairs)[0]
    for w2 in sq:
        shell = np.floor(np.sqrt((radii + w2).astype(np.float64)) + 0.5).astype(np.int64)
        counts += np.bincount(shell, weights=pairs[radii], minlength=K)[:K]
    return fwd, np.ascontiguousarray(inv), np.maximum(counts, 1.0).astype(np.float32).reshape(1, K)


VMEM = pl.BlockSpec(memory_space=pltpu.VMEM)
HBM = pl.BlockSpec(memory_space=pltpu.HBM)


def body(spectral_field, fwd, inv, counts):
    updated, spectrum = pl.pallas_call(
        transform_kernel,
        out_shape=(
            jax.ShapeDtypeStruct((2, 8, 32, 256), F32),
            jax.ShapeDtypeStruct((1, 256), F32),
        ),
        in_specs=[HBM, HBM, HBM, VMEM],
        out_specs=(VMEM, VMEM),
        scratch_shapes=[
            pltpu.VMEM((2, 8, 32, 256), F32),
            pltpu.VMEM((512, 512), BF16),
            pltpu.VMEM((512, 512), BF16),
            pltpu.VMEM((512, 512), BF16),
            pltpu.VMEM((256, 256), BF16),
            pltpu.VMEM((1024, 1024), BF16),
            pltpu.VMEM((4, 8, 2, 16, 256), BF16),
            pltpu.VMEM((4, 8, 2, 16, 256), BF16),
            pltpu.VMEM((2, 8, 16, 256), BF16),
            pltpu.VMEM((8, 2, 4, 8, 8, 128), BF16),
            pltpu.VMEM((8, 2, 4, 8, 8, 128), BF16),
            pltpu.VMEM((8, 4, 8, 8, 256), BF16),
            pltpu.VMEM((512, 256), BF16),
            pltpu.VMEM((8, 4, 8, 2, 8, 128), BF16),
            pltpu.VMEM((8, 4, 8, 2, 8, 128), BF16),
            pltpu.VMEM((4, 8, 2, 32, 128), BF16),
            pltpu.VMEM((4, 8, 2, 32, 128), BF16),
            pltpu.VMEM((2, 8, 32, 512), BF16),
            pltpu.VMEM((1, 256), F32),
            pltpu.VMEM((32, 1, 256), F32),
            pltpu.VMEM((8, 1, 256), F32),
            pltpu.VMEM((1, 256), F32),
        ] + [pltpu.SemaphoreType.DMA((4, 8))] * 8 + [
            pltpu.SemaphoreType.DMA((3,)),
            pltpu.SemaphoreType.DMA((32,)),
            pltpu.SemaphoreType.DMA((32,)),
            pltpu.SemaphoreType.DMA((8,)),
            pltpu.SemaphoreType.DMA((8,)),
        ],
        compiler_params=pltpu.CompilerParams(
            collective_id=0, has_side_effects=True, vmem_limit_bytes=67000000),
        name="transforms",
    )(spectral_field, fwd, inv, counts)
    return updated, spectrum.reshape(256)


def solution(mesh):
    fwd, inv, counts = tables()
    step = functools.partial(jax.shard_map, mesh=mesh, check_vma=False)

    def run(spectral_field):
        return step(
            lambda f: body(f, jnp.asarray(fwd), jnp.asarray(inv), jnp.asarray(counts)),
            in_specs=(P(None, "row", "col", None),),
            out_specs=(P(None, "row", "col", None), P()),
        )(spectral_field)

    return run
```

```python
import functools
import math

import jax
import jax.numpy as jnp
import numpy as np
from jax import lax
from jax.experimental import pallas as pl
from jax.experimental.pallas import tpu as pltpu
from jax.sharding import PartitionSpec as P

PHASE_RATE = 0.0002
COUPLING = 0.2
K = 256
N = 512
BF16 = jnp.bfloat16
F32 = jnp.float32


def mm(a, b):
    return lax.dot_general(a, b, (((1,), (0,)), ((), ())), preferred_element_type=F32)


def mmt(a, b):
    return lax.dot_general(a, b, (((1,), (1,)), ((), ())), preferred_element_type=F32)


def iota(shape, dim):
    return lax.broadcasted_iota(jnp.int32, shape, dim)


def one_hot(hit):
    return jnp.where(hit, 1.0, 0.0).astype(BF16)


def shell_sums(energy, r2):
    j = jnp.abs(iota((256, 128), 0) - 128)
    within = jnp.where(j <= iota((256, 128), 1), 1.0, 0.0)
    prefix = lax.dot_general(energy, within, (((1,), (0,)), ((), ())),
                             preferred_element_type=F32, precision=lax.Precision.HIGHEST)
    parts = []
    for t in range(2):
        s = iota((1, 128), 1) + t * 128
        room = s * s + s - r2
        m = jnp.sqrt(jnp.maximum(room, 0).astype(F32) + 0.5).astype(jnp.int32)
        inner = jnp.take_along_axis(prefix, jnp.minimum(m, 127), axis=1, mode="promise_in_bounds")
        total = jnp.where(room >= 0, inner, 0.0) + jnp.where(room >= 128 * 128, energy[:, :1], 0.0)
        parts.append(jnp.sum(total, axis=0, keepdims=True))
    lane = iota((1, 256), 1)
    shifted = jnp.concatenate([pltpu.roll(parts[0], 1, 1), pltpu.roll(parts[1], 1, 1)], axis=1)
    shifted = jnp.where(lane == 0, 0.0, jnp.where(lane == 128, parts[0][:, 127:], shifted))
    return jnp.concatenate(parts, axis=1) - shifted


def transform_kernel(
    field_hbm, fwd_hbm, inv_hbm, last_hbm, counts, out, spectrum,
    field, fwd, inv, last, p1, p2, p3, aout, bin_, yb, bout, cin, cub, cout, din, dout, ein, zb,
    shells, first, second, mid,
    s1, r1, s2, r2, s3, r3, s4, r4, load_sem, s5, r5, s6, r6,
):
    row = lax.axis_index("row")
    xh = lax.axis_index("col")
    zl = row // 8
    yc = row % 8

    def remote(src, dst, send, recv, to_row, to_col):
        return pltpu.make_async_remote_copy(
            src_ref=src, dst_ref=dst, send_sem=send, recv_sem=recv,
            device_id={"row": to_row, "col": to_col}, device_id_type=pl.DeviceIdType.MESH,
        )

    loads = [
        pltpu.make_async_copy(field_hbm, field, load_sem.at[0]),
        pltpu.make_async_copy(inv_hbm, inv, load_sem.at[1]),
        pltpu.make_async_copy(fwd_hbm, fwd, load_sem.at[2]),
        pltpu.make_async_copy(last_hbm, last, load_sem.at[3]),
    ]
    for load in loads:
        load.start()

    barrier = pltpu.get_barrier_semaphore()

    @pl.loop(1, 32)
    def _(i):
        d = (zl * 8 + xh + i) % 32
        pl.semaphore_signal(
            barrier, inc=1, device_id={"row": (d // 8) * 8 + yc, "col": d % 8},
            device_id_type=pl.DeviceIdType.MESH,
        )

    @pl.loop(1, 8)
    def _(j):
        pl.semaphore_signal(
            barrier, inc=1, device_id={"row": zl * 8 + (yc + j) % 8, "col": xh},
            device_id_type=pl.DeviceIdType.MESH,
        )

    def copy1(h, k, i):
        zd = (zl + 4 - k) % 4
        xd = (xh + i) % 8
        return remote(aout.at[h, zd, xd], bin_.at[h, zl, xh], s1.at[h, k, i], r1.at[h, k, i], zd * 8 + yc, xd)

    def copy2(h, k, j):
        zs = (zl + k) % 4
        yd = (yc + j) % 8
        return remote(bout.at[h, yd, zs], cin.at[h, zs, yc], s2.at[h, k, j], r2.at[h, k, j], zl * 8 + yd, xh)

    def copy3(h, k, j):
        zs = (zl + k) % 4
        yd = (yc + j) % 8
        return remote(cout.at[h, yd, zs], din.at[h, yc, zs], s3.at[h, k, j], r3.at[h, k, j], zl * 8 + yd, xh)

    def copy4(h, k, i):
        zd = (zl + k) % 4
        xd = (xh + i) % 8
        return remote(dout.at[h, zd, xd], ein.at[h, zl, xh], s4.at[h, k, i], r4.at[h, k, i], zd * 8 + yc, xd)

    me1 = zl * 8 + xh

    def copy5(i):
        d = (me1 + i) % 32
        return remote(shells, first.at[me1], s5.at[i], r5.at[i], (d // 8) * 8 + yc, d % 8)

    def copy6(j):
        return remote(mid, second.at[yc], s6.at[j], r6.at[j], zl * 8 + (yc + j) % 8, xh)

    j1 = iota((128, 512), 1)
    f1 = ((j1 // 32) % 4) * 128 + (j1 // 128) * 32 + j1 % 32

    @pl.loop(0, 4)
    def _(b):
        rows = pl.ds(pl.multiple_of(b * 128, 128), 128)
        p1[rows, :] = one_hot(iota((128, 512), 0) + b * 128 == f1)

    q2 = iota((128, 128), 0)
    p2[...] = one_hot(iota((128, 128), 1) == (q2 // 64) * 64 + (q2 % 8) * 8 + (q2 // 8) % 8)

    j3 = iota((128, 1024), 1)
    f3 = ((j3 // 8) % 8) * 128 + ((j3 // 64) % 2) * 64 + (j3 % 8) * 8 + j3 // 128

    @pl.loop(0, 8)
    def _(b):
        rows = pl.ds(pl.multiple_of(b * 128, 128), 128)
        p3[rows, :] = one_hot(iota((128, 1024), 0) + b * 128 == f3)

    loads[0].wait()
    loads[1].wait()

    @pl.loop(0, 4)
    def _(zd):
        rows = pl.ds(pl.multiple_of(zd * 128, 128), 128)
        c, s = inv[rows, :256], inv[rows, 256:]
        re = field[0].reshape(256, 256).astype(BF16)
        im = field[1].reshape(256, 256).astype(BF16)
        pair = (
            (mmt(c, re) - mmt(s, im)) * (1.0 / 16.0),
            (mmt(s, re) + mmt(c, im)) * (1.0 / 16.0),
        )
        for ri in range(2):
            v = pair[ri].reshape(8, 2, 8, 256)
            for h in range(2):
                aout[h, zd, :, ri] = v[:, h].astype(BF16)

    for h in range(2):
        bin_[h, zl, xh] = aout[h, zl, xh]
    pl.semaphore_wait(barrier, 38)

    @pl.loop(0, 2)
    def _(h):
        @pl.loop(1, 8)
        def _(i):
            copy1(h, 0, i).start()

        @pl.loop(1, 4)
        def _(k):
            @pl.loop(0, 8)
            def _(i):
                copy1(h, k, i).start()

    loads[2].wait()
    loads[3].wait()

    def stage_b(h, k):
        zs = (zl + k) % 4
        parts = []
        for ht in range(2):
            for xt in range(2):
                lanes = slice(xt * 128, xt * 128 + 128)
                parts.append(jnp.concatenate(
                    [bin_[h, zs, ht * 4 + q, :, :, lanes].reshape(16, 128) for q in range(4)], axis=1))
        o = mm(jnp.concatenate(parts, axis=0), p1[...])
        for ht in range(2):
            for xt in range(2):
                base = (ht * 2 + xt) * 16
                for c in range(2):
                    for x in range(4):
                        yb[c, xt * 4 + x, :, ht * 128:ht * 128 + 128] = (
                            o[base + c * 8:base + c * 8 + 8, x * 128:x * 128 + 128].astype(BF16))
        q = mm(p2[...], yb[...].reshape(128, 256)).astype(BF16)
        mc = mm(q, fwd[:256, :])
        ms = mm(q, fwd[256:, :])
        pair = ((mc[:64] - ms[64:]) * (1.0 / 16.0), (ms[:64] + mc[64:]) * (1.0 / 16.0))
        for c in range(2):
            for y in range(4):
                w = pair[c][:, y * 128:y * 128 + 128].reshape(2, 4, 8, 128)
                for zh in range(2):
                    bout[h, y * 2 + zh, zs, :, c] = w[zh].astype(BF16)
        cin[h, zs, yc] = bout[h, yc, zs]

    @pl.loop(0, 2)
    def _(h):
        @pl.loop(0, 4)
        def _(k):
            @pl.when(k > 0)
            def _():
                copy1(h, k, 0).wait_recv()

            @pl.loop(1, 8)
            def _(i):
                copy1(h, k, i).wait_recv()

            stage_b(h, k)

            @pl.loop(1, 8)
            def _(j):
                copy2(h, k, j).start()

    def stage_c(h, z, slot):
        d = jnp.concatenate([cin[h, :, :, z, 0].reshape(256, 128), cin[h, :, :, z, 1].reshape(256, 128)], axis=1)
        d = jnp.concatenate([d, jnp.concatenate([-d[:, 128:], d[:, :128]], axis=1)], axis=0)
        for half in range(2):
            rows = slice(half * 256, half * 256 + 256)
            phys = mm(inv[rows, :], d) * (1.0 / 16.0)
            re, im = phys[:, :128], phys[:, 128:]
            gain = COUPLING * (re * re + im * im)
            cub[slot, rows, :128] = (gain * re).astype(BF16)
            cub[slot, rows, 128:] = (gain * im).astype(BF16)

    def stage_c_back(h, z, slot):
        m = mm(fwd[...], cub[slot])
        pair = (
            (m[:256, :128] + m[256:, 128:]) * (1.0 / 32.0),
            (m[:256, 128:] - m[256:, :128]) * (1.0 / 32.0),
        )
        for c in range(2):
            v = pair[c].reshape(4, 8, 8, 128)
            for q in range(4):
                cout[h, :, q, z, c] = v[q].astype(BF16)

    @pl.loop(0, 2)
    def _(h):
        @pl.loop(0, 4)
        def _(k):
            @pl.loop(1, 8)
            def _(j):
                copy2(h, k, j).wait_recv()

        @pl.loop(0, 2)
        def _(z):
            stage_c(h, 2 * z, 0)
            stage_c(h, 2 * z + 1, 1)
            stage_c_back(h, 2 * z, 0)
            stage_c_back(h, 2 * z + 1, 1)

        @pl.loop(0, 4)
        def _(k):
            @pl.loop(1, 8)
            def _(j):
                copy3(h, k, j).start()

        din[h, yc] = cout[h, yc]

    def stage_d(h, k):
        zs = (zl + k) % 4
        r = []
        for c in range(2):
            r.append(jnp.concatenate([
                jnp.concatenate([din[h, y * 2 + zh, zs, :, c].reshape(32, 128) for zh in range(2)], axis=0)
                for y in range(4)], axis=1))
        o = mmt(fwd[:256, :], jnp.concatenate(r, axis=0)) + mmt(fwd[256:, :], jnp.concatenate([r[1], -r[0]], axis=0))
        dout[h, zs] = (o * (1.0 / 32.0)).astype(BF16).reshape(8, 32, 128)

    @pl.loop(0, 2)
    def _(h):
        @pl.loop(0, 4)
        def _(k):
            @pl.loop(1, 8)
            def _(j):
                copy3(h, k, j).wait_recv()

            stage_d(h, k)

            @pl.when(k > 0)
            def _():
                copy4(h, k, 0).start()

            @pl.loop(1, 8)
            def _(i):
                copy4(h, k, i).start()

        ein[h, zl, xh] = dout[h, zl, xh]

    for h in range(2):
        @pl.loop(0, 4)
        def _(k, h=h):
            @pl.when(k > 0)
            def _():
                copy4(h, k, 0).wait_recv()

            @pl.loop(1, 8)
            def _(i):
                copy4(h, k, i).wait_recv()

        parts = [jnp.concatenate([ein[h, g, s] for s in range(8)], axis=1) for g in range(4)]
        o = mm(jnp.concatenate(parts, axis=0), p3[...]).astype(BF16)
        for g in range(4):
            for x in range(8):
                zb[x, :, (h * 4 + g) * 128:(h * 4 + g) * 128 + 128] = o[g * 32:g * 32 + 32, x * 128:x * 128 + 128]
    nl = mm(zb[...].reshape(256, 1024), last[...]) * (1.0 / 32.0)
    nl_re, nl_im = nl[:, :256], nl[:, 256:]
    u = field[0].reshape(256, 256) - nl_im
    v = field[1].reshape(256, 256) + nl_re
    out[0] = u.reshape(8, 32, 256)
    out[1] = v.reshape(8, 32, 256)

    wz = iota((1, 256), 1) - 128
    r = iota((256, 1), 0)
    wx = row * 8 - 128 + r // 32
    wy = xh * 32 - 128 + r % 32
    rad2 = wx * wx + wy * wy
    shells[...] = shell_sums(u * u + v * v, rad2)
    first[me1] = shells[...]

    @pl.loop(1, 32)
    def _(i):
        copy5(i).start()

    az = PHASE_RATE * (wz * wz).astype(F32)
    ar = PHASE_RATE * rad2.astype(F32)
    cz, sz = jnp.cos(az), jnp.sin(az)
    cr, sr = jnp.cos(ar), jnp.sin(ar)
    cos = (cr * cz - sr * sz).reshape(8, 32, 256)
    sin = (sr * cz + cr * sz).reshape(8, 32, 256)
    u, v = out[0], out[1]
    out[0] = u * cos + v * sin
    out[1] = v * cos - u * sin

    @pl.loop(1, 32)
    def _(i):
        copy5(i).wait_recv()

    mid[...] = jnp.sum(first[...], axis=0)
    second[yc] = mid[...]

    @pl.loop(1, 8)
    def _(j):
        copy6(j).start()

    @pl.loop(1, 8)
    def _(j):
        copy6(j).wait_recv()

    spectrum[...] = jnp.sum(second[...], axis=0) / counts[...]

    @pl.loop(0, 2)
    def _(h):
        @pl.loop(0, 4)
        def _(k):
            @pl.when(k > 0)
            def _():
                copy1(h, k, 0).wait_send()
                copy4(h, k, 0).wait_send()

            @pl.loop(1, 8)
            def _(i):
                copy1(h, k, i).wait_send()
                copy2(h, k, i).wait_send()
                copy3(h, k, i).wait_send()
                copy4(h, k, i).wait_send()

    @pl.loop(1, 32)
    def _(i):
        copy5(i).wait_send()

    @pl.loop(1, 8)
    def _(j):
        copy6(j).wait_send()


def tables():
    waves = np.arange(K, dtype=np.int64) - K // 2
    phase = (waves[:, None] * np.arange(N, dtype=np.int64)[None, :]) % N
    angle = phase.astype(np.float32) * np.float32(2.0 * math.pi / N)
    cos = np.cos(angle).astype(jnp.bfloat16)
    sin = np.sin(angle).astype(jnp.bfloat16)
    fwd = np.concatenate([cos, sin], axis=0)
    inv = np.concatenate([cos.T, sin.T], axis=1)
    h, g, c, s, z = np.meshgrid(*(np.arange(n) for n in (2, 4, 2, 8, 8)), indexing="ij")
    point = ((g * 8 + s) * 16 + h * 8 + z).reshape(-1)
    is_re = (c.reshape(-1) == 0)[:, None]
    ct, st = cos.T[point], sin.T[point]
    last = np.concatenate([np.where(is_re, ct, st), np.where(is_re, -st, ct)], axis=1)
    sq = waves * waves
    q = (sq[:, None] + sq[None, :]).reshape(-1)
    pairs = np.bincount(q, minlength=2 * (K // 2) ** 2 + 1)
    counts = np.zeros(K, np.float64)
    radii = np.nonzero(pairs)[0]
    for w2 in sq:
        shell = np.floor(np.sqrt((radii + w2).astype(np.float64)) + 0.5).astype(np.int64)
        counts += np.bincount(shell, weights=pairs[radii], minlength=K)[:K]
    return fwd, np.ascontiguousarray(inv), last, np.maximum(counts, 1.0).astype(np.float32).reshape(1, K)


VMEM = pl.BlockSpec(memory_space=pltpu.VMEM)
HBM = pl.BlockSpec(memory_space=pltpu.HBM)


def body(spectral_field, fwd, inv, last, counts):
    updated, spectrum = pl.pallas_call(
        transform_kernel,
        out_shape=(
            jax.ShapeDtypeStruct((2, 8, 32, 256), F32),
            jax.ShapeDtypeStruct((1, 256), F32),
        ),
        in_specs=[HBM, HBM, HBM, HBM, VMEM],
        out_specs=(VMEM, VMEM),
        scratch_shapes=[
            pltpu.VMEM((2, 8, 32, 256), F32),
            pltpu.VMEM((512, 512), BF16),
            pltpu.VMEM((512, 512), BF16),
            pltpu.VMEM((1024, 512), BF16),
            pltpu.VMEM((512, 512), BF16),
            pltpu.VMEM((128, 128), BF16),
            pltpu.VMEM((1024, 1024), BF16),
            pltpu.VMEM((2, 4, 8, 2, 8, 256), BF16),
            pltpu.VMEM((2, 4, 8, 2, 8, 256), BF16),
            pltpu.VMEM((2, 8, 8, 256), BF16),
            pltpu.VMEM((2, 8, 4, 4, 2, 8, 128), BF16),
            pltpu.VMEM((2, 4, 8, 4, 2, 8, 128), BF16),
            pltpu.VMEM((2, 512, 256), BF16),
            pltpu.VMEM((2, 8, 4, 4, 2, 8, 128), BF16),
            pltpu.VMEM((2, 8, 4, 4, 2, 8, 128), BF16),
            pltpu.VMEM((2, 4, 8, 32, 128), BF16),
            pltpu.VMEM((2, 4, 8, 32, 128), BF16),
            pltpu.VMEM((8, 32, 1024), BF16),
            pltpu.VMEM((1, 256), F32),
            pltpu.VMEM((32, 1, 256), F32),
            pltpu.VMEM((8, 1, 256), F32),
            pltpu.VMEM((1, 256), F32),
        ] + [pltpu.SemaphoreType.DMA((2, 4, 8))] * 8 + [
            pltpu.SemaphoreType.DMA((4,)),
            pltpu.SemaphoreType.DMA((32,)),
            pltpu.SemaphoreType.DMA((32,)),
            pltpu.SemaphoreType.DMA((8,)),
            pltpu.SemaphoreType.DMA((8,)),
        ],
        compiler_params=pltpu.CompilerParams(
            collective_id=0, has_side_effects=True, vmem_limit_bytes=67000000),
        name="transforms",
    )(spectral_field, fwd, inv, last, counts)
    return updated, spectrum.reshape(256)


def solution(mesh):
    consts = tables()
    step = functools.partial(jax.shard_map, mesh=mesh, check_vma=False)

    def run(spectral_field):
        return step(
            lambda f: body(f, *(jnp.asarray(c) for c in consts)),
            in_specs=(P(None, "row", "col", None),),
            out_specs=(P(None, "row", "col", None), P()),
        )(spectral_field)

    return run
```

```python
import functools
import math

import jax
import jax.numpy as jnp
import numpy as np
from jax import lax
from jax.experimental import pallas as pl
from jax.experimental.pallas import tpu as pltpu
from jax.sharding import PartitionSpec as P

PHASE_RATE = 0.0002
COUPLING = 0.2
K = 256
N = 512
BF16 = jnp.bfloat16
F32 = jnp.float32


def mm(a, b):
    return lax.dot_general(a, b, (((1,), (0,)), ((), ())), preferred_element_type=F32)


def mmt(a, b):
    return lax.dot_general(a, b, (((1,), (1,)), ((), ())), preferred_element_type=F32)


def iota(shape, dim):
    return lax.broadcasted_iota(jnp.int32, shape, dim)


def one_hot(hit):
    return jnp.where(hit, 1.0, 0.0).astype(BF16)


def shell_room(rad2, part):
    s = iota((1, 128), 1) + part * 128
    return s * s + s - rad2


def shell_reach(rad2, part):
    room = jnp.maximum(shell_room(rad2, part), 0).astype(F32)
    return jnp.minimum(jnp.sqrt(room + 0.5).astype(jnp.int32), 127)


def shell_sums(energy, rad2, reach):
    j = jnp.abs(iota((256, 128), 0) - 128)
    within = jnp.where(j <= iota((256, 128), 1), 1.0, 0.0)
    prefix = lax.dot_general(energy, within, (((1,), (0,)), ((), ())),
                             preferred_element_type=F32, precision=lax.Precision.HIGHEST)
    parts = []
    for part in range(2):
        room = shell_room(rad2, part)
        inner = jnp.take_along_axis(prefix, reach[part], axis=1, mode="promise_in_bounds")
        total = jnp.where(room >= 0, inner, 0.0) + jnp.where(room >= 128 * 128, energy[:, :1], 0.0)
        parts.append(jnp.sum(total, axis=0, keepdims=True))
    lane = iota((1, 256), 1)
    shifted = jnp.concatenate([pltpu.roll(parts[0], 1, 1), pltpu.roll(parts[1], 1, 1)], axis=1)
    shifted = jnp.where(lane == 0, 0.0, jnp.where(lane == 128, parts[0][:, 127:], shifted))
    return jnp.concatenate(parts, axis=1) - shifted


def transform_kernel(
    field_hbm, fwd_hbm, inv_hbm, last_hbm, counts_hbm, out, spectrum,
    field, fwd, inv, last, counts, p1, p2, p3, aout, bin_, yb, bout, cin, cub, cout, din, dout, ein, zb, reach,
    shells, first, second, mid,
    s1, r1, s2, r2, s3, r3, s4, r4, load_sem, s5, r5, s6, r6,
):
    row = lax.axis_index("row")
    xh = lax.axis_index("col")
    zl = row // 8
    yc = row % 8

    def remote(src, dst, send, recv, to_row, to_col):
        return pltpu.make_async_remote_copy(
            src_ref=src, dst_ref=dst, send_sem=send, recv_sem=recv,
            device_id={"row": to_row, "col": to_col}, device_id_type=pl.DeviceIdType.MESH,
        )

    loads = [
        pltpu.make_async_copy(field_hbm, field, load_sem.at[0]),
        pltpu.make_async_copy(inv_hbm, inv, load_sem.at[1]),
        pltpu.make_async_copy(fwd_hbm, fwd, load_sem.at[2]),
        pltpu.make_async_copy(last_hbm, last, load_sem.at[3]),
        pltpu.make_async_copy(counts_hbm, counts, load_sem.at[4]),
    ]
    for load in loads:
        load.start()

    barrier = pltpu.get_barrier_semaphore()

    @pl.loop(1, 32)
    def _(i):
        d = (zl * 8 + xh + i) % 32
        pl.semaphore_signal(
            barrier, inc=1, device_id={"row": (d // 8) * 8 + yc, "col": d % 8},
            device_id_type=pl.DeviceIdType.MESH,
        )

    @pl.loop(1, 8)
    def _(j):
        pl.semaphore_signal(
            barrier, inc=1, device_id={"row": zl * 8 + (yc + j) % 8, "col": xh},
            device_id_type=pl.DeviceIdType.MESH,
        )

    def wait(ref, sem):
        pltpu.make_async_copy(ref, ref, sem).wait()

    def copy1(h, k, i):
        zd = (zl + 6 - k) % 4
        xd = (xh + i) % 8
        return remote(aout.at[h, zd, xd], bin_.at[h, zl, xh], s1.at[h, k], r1.at[h, k], zd * 8 + yc, xd)

    def copy2(h, k, j):
        zs = (zl + k + 2) % 4
        yd = (yc + j) % 8
        return remote(bout.at[h, yd, zs], cin.at[h, zs, yc], s2.at[h, k], r2.at[h, k], zl * 8 + yd, xh)

    def copy3(h, k, j):
        zs = (zl + k + 3) % 4
        yd = (yc + j) % 8
        return remote(cout.at[h, yd, zs], din.at[h, yc, zs], s3.at[h, k], r3.at[h, k], zl * 8 + yd, xh)

    def copy4(h, k, i):
        zd = (zl + k + 3) % 4
        xd = (xh + i) % 8
        return remote(dout.at[h, zd, xd], ein.at[h, zl, xh], s4.at[h, k], r4.at[h, k], zd * 8 + yc, xd)

    def start_all(copy, h, k, own):
        @pl.when(k != own)
        def _():
            copy(h, k, 0).start()

        @pl.loop(1, 8)
        def _(i):
            copy(h, k, i).start()

    def wait_all(ref, sem, h, k, own):
        @pl.when(k != own)
        def _():
            wait(ref.at[h, 0], sem.at[h, k])

        @pl.when(k == own)
        def _():
            wait(ref.at[h, 0, pl.ds(0, 7)], sem.at[h, k])

    me1 = zl * 8 + xh

    def copy5(i):
        d = (me1 + i) % 32
        return remote(shells, first.at[me1], s5.at[0], r5.at[0], (d // 8) * 8 + yc, d % 8)

    def copy6(j):
        return remote(mid, second.at[yc], s6.at[0], r6.at[0], zl * 8 + (yc + j) % 8, xh)

    j1 = iota((128, 512), 1)
    f1 = ((j1 // 32) % 4) * 128 + (j1 // 128) * 32 + j1 % 32

    @pl.loop(0, 4)
    def _(b):
        rows = pl.ds(pl.multiple_of(b * 128, 128), 128)
        p1[rows, :] = one_hot(iota((128, 512), 0) + b * 128 == f1)

    q2 = iota((128, 128), 0)
    p2[...] = one_hot(iota((128, 128), 1) == (q2 // 64) * 64 + (q2 % 8) * 8 + (q2 // 8) % 8)

    j3 = iota((128, 1024), 1)
    f3 = ((j3 // 8) % 8) * 128 + ((j3 // 64) % 2) * 64 + (j3 % 8) * 8 + j3 // 128

    @pl.loop(0, 8)
    def _(b):
        rows = pl.ds(pl.multiple_of(b * 128, 128), 128)
        p3[rows, :] = one_hot(iota((128, 1024), 0) + b * 128 == f3)

    loads[0].wait()
    loads[1].wait()

    @pl.loop(0, 4)
    def _(zd):
        rows = pl.ds(pl.multiple_of(zd * 128, 128), 128)
        c, s = inv[rows, :256], inv[rows, 256:]
        re = field[0].reshape(256, 256).astype(BF16)
        im = field[1].reshape(256, 256).astype(BF16)
        pair = (
            (mmt(c, re) - mmt(s, im)) * (1.0 / 16.0),
            (mmt(s, re) + mmt(c, im)) * (1.0 / 16.0),
        )
        for ri in range(2):
            v = pair[ri].reshape(8, 2, 8, 256)
            for h in range(2):
                aout[h, zd, :, ri] = v[:, h].astype(BF16)

    for h in range(2):
        bin_[h, zl, xh] = aout[h, zl, xh]
    pl.semaphore_wait(barrier, 38)

    @pl.loop(0, 2)
    def _(h):
        @pl.loop(0, 4)
        def _(k):
            start_all(copy1, h, k, 2)

    wz = iota((1, 256), 1) - 128
    r = iota((256, 1), 0)
    wx = row * 8 - 128 + r // 32
    wy = xh * 32 - 128 + r % 32
    rad2 = wx * wx + wy * wy
    for part in range(2):
        reach[part] = shell_reach(rad2, part)

    loads[2].wait()
    loads[3].wait()
    loads[4].wait()

    def stage_b(h, k):
        zs = (zl + k + 2) % 4
        parts = []
        for ht in range(2):
            for xt in range(2):
                lanes = slice(xt * 128, xt * 128 + 128)
                parts.append(jnp.concatenate(
                    [bin_[h, zs, ht * 4 + q, :, :, lanes].reshape(16, 128) for q in range(4)], axis=1))
        o = mm(jnp.concatenate(parts, axis=0), p1[...])
        for ht in range(2):
            for xt in range(2):
                base = (ht * 2 + xt) * 16
                for c in range(2):
                    for x in range(4):
                        yb[c, xt * 4 + x, :, ht * 128:ht * 128 + 128] = (
                            o[base + c * 8:base + c * 8 + 8, x * 128:x * 128 + 128].astype(BF16))
        q = mm(p2[...], yb[...].reshape(128, 256)).astype(BF16)
        mc = mm(q, fwd[:256, :])
        ms = mm(q, fwd[256:, :])
        pair = ((mc[:64] - ms[64:]) * (1.0 / 16.0), (ms[:64] + mc[64:]) * (1.0 / 16.0))
        for c in range(2):
            for y in range(4):
                w = pair[c][:, y * 128:y * 128 + 128].reshape(2, 4, 8, 128)
                for zh in range(2):
                    bout[h, y * 2 + zh, zs, :, c] = w[zh].astype(BF16)
        cin[h, zs, yc] = bout[h, yc, zs]

    @pl.loop(0, 2)
    def _(h):
        @pl.loop(0, 4)
        def _(k):
            wait_all(bin_, r1, h, k, 2)
            stage_b(h, k)

            @pl.loop(1, 8)
            def _(j):
                copy2(h, k, j).start()

    def stage_c(h, z, slot):
        d = jnp.concatenate([cin[h, :, :, z, 0].reshape(256, 128), cin[h, :, :, z, 1].reshape(256, 128)], axis=1)
        d = jnp.concatenate([d, jnp.concatenate([-d[:, 128:], d[:, :128]], axis=1)], axis=0)
        for half in range(2):
            rows = slice(half * 256, half * 256 + 256)
            phys = mm(inv[rows, :], d) * (1.0 / 16.0)
            re, im = phys[:, :128], phys[:, 128:]
            gain = COUPLING * (re * re + im * im)
            cub[slot, rows, :128] = (gain * re).astype(BF16)
            cub[slot, rows, 128:] = (gain * im).astype(BF16)

    def stage_c_back(h, z, slot):
        m = mm(fwd[...], cub[slot])
        pair = (
            (m[:256, :128] + m[256:, 128:]) * (1.0 / 32.0),
            (m[:256, 128:] - m[256:, :128]) * (1.0 / 32.0),
        )
        for c in range(2):
            v = pair[c].reshape(4, 8, 8, 128)
            for q in range(4):
                cout[h, :, q, z, c] = v[q].astype(BF16)

    @pl.loop(0, 2)
    def _(h):
        @pl.loop(0, 4)
        def _(k):
            wait(cin.at[h, 0, pl.ds(0, 7)], r2.at[h, k])

        @pl.loop(0, 2)
        def _(z):
            stage_c(h, 2 * z, 0)
            stage_c(h, 2 * z + 1, 1)
            stage_c_back(h, 2 * z, 0)
            stage_c_back(h, 2 * z + 1, 1)

        @pl.loop(0, 4)
        def _(k):
            @pl.loop(1, 8)
            def _(j):
                copy3(h, k, j).start()

        din[h, yc] = cout[h, yc]

    def stage_d(h, k):
        zs = (zl + k + 3) % 4
        r = []
        for c in range(2):
            r.append(jnp.concatenate([
                jnp.concatenate([din[h, y * 2 + zh, zs, :, c].reshape(32, 128) for zh in range(2)], axis=0)
                for y in range(4)], axis=1))
        o = mmt(fwd[:256, :], jnp.concatenate(r, axis=0)) + mmt(fwd[256:, :], jnp.concatenate([r[1], -r[0]], axis=0))
        dout[h, zs] = (o * (1.0 / 32.0)).astype(BF16).reshape(8, 32, 128)

    @pl.loop(0, 2)
    def _(h):
        @pl.loop(0, 4)
        def _(k):
            wait(din.at[h, pl.ds(0, 7), 0], r3.at[h, k])
            stage_d(h, k)
            start_all(copy4, h, k, 1)

        ein[h, zl, xh] = dout[h, zl, xh]

    for h in range(2):
        @pl.loop(0, 4)
        def _(k, h=h):
            wait_all(ein, r4, h, k, 1)

        parts = [jnp.concatenate([ein[h, g, s] for s in range(8)], axis=1) for g in range(4)]
        o = mm(jnp.concatenate(parts, axis=0), p3[...]).astype(BF16)
        for g in range(4):
            for x in range(8):
                zb[h, x, :, g * 128:g * 128 + 128] = o[g * 32:g * 32 + 32, x * 128:x * 128 + 128]
        nl = mm(zb[h].reshape(256, 512), last[h * 512:h * 512 + 512, :]) * (1.0 / 32.0)
        base = field if h == 0 else out
        u = base[0].reshape(256, 256) - nl[:, 256:]
        v = base[1].reshape(256, 256) + nl[:, :256]
        out[0] = u.reshape(8, 32, 256)
        out[1] = v.reshape(8, 32, 256)

    shells[...] = shell_sums(u * u + v * v, rad2, reach)
    first[me1] = shells[...]

    @pl.loop(1, 32)
    def _(i):
        copy5(i).start()

    az = PHASE_RATE * (wz * wz).astype(F32)
    ar = PHASE_RATE * rad2.astype(F32)
    cz, sz = jnp.cos(az), jnp.sin(az)
    cr, sr = jnp.cos(ar), jnp.sin(ar)
    cos = (cr * cz - sr * sz).reshape(8, 32, 256)
    sin = (sr * cz + cr * sz).reshape(8, 32, 256)
    u, v = out[0], out[1]
    out[0] = u * cos + v * sin
    out[1] = v * cos - u * sin

    wait(first.at[pl.ds(0, 31)], r5.at[0])

    mid[...] = jnp.sum(first[...], axis=0)
    second[yc] = mid[...]

    @pl.loop(1, 8)
    def _(j):
        copy6(j).start()

    wait(second.at[pl.ds(0, 7)], r6.at[0])

    spectrum[...] = jnp.sum(second[...], axis=0) / counts[...]

    @pl.loop(0, 2)
    def _(h):
        @pl.loop(0, 4)
        def _(k):
            wait_all(aout, s1, h, k, 2)
            wait(bout.at[h, pl.ds(0, 7), 0], s2.at[h, k])
            wait(cout.at[h, pl.ds(0, 7), 0], s3.at[h, k])
            wait_all(dout, s4, h, k, 1)

    wait(first.at[pl.ds(0, 31)], s5.at[0])
    wait(second.at[pl.ds(0, 7)], s6.at[0])


def tables():
    waves = np.arange(K, dtype=np.int64) - K // 2
    phase = (waves[:, None] * np.arange(N, dtype=np.int64)[None, :]) % N
    angle = phase.astype(np.float32) * np.float32(2.0 * math.pi / N)
    cos = np.cos(angle).astype(jnp.bfloat16)
    sin = np.sin(angle).astype(jnp.bfloat16)
    fwd = np.concatenate([cos, sin], axis=0)
    inv = np.concatenate([cos.T, sin.T], axis=1)
    h, g, c, s, z = np.meshgrid(*(np.arange(n) for n in (2, 4, 2, 8, 8)), indexing="ij")
    point = ((g * 8 + s) * 16 + h * 8 + z).reshape(-1)
    is_re = (c.reshape(-1) == 0)[:, None]
    ct, st = cos.T[point], sin.T[point]
    last = np.concatenate([np.where(is_re, ct, st), np.where(is_re, -st, ct)], axis=1)
    sq = waves * waves
    q = (sq[:, None] + sq[None, :]).reshape(-1)
    pairs = np.bincount(q, minlength=2 * (K // 2) ** 2 + 1)
    counts = np.zeros(K, np.float64)
    radii = np.nonzero(pairs)[0]
    for w2 in sq:
        shell = np.floor(np.sqrt((radii + w2).astype(np.float64)) + 0.5).astype(np.int64)
        counts += np.bincount(shell, weights=pairs[radii], minlength=K)[:K]
    return fwd, np.ascontiguousarray(inv), last, np.maximum(counts, 1.0).astype(np.float32).reshape(1, K)


VMEM = pl.BlockSpec(memory_space=pltpu.VMEM)
HBM = pl.BlockSpec(memory_space=pltpu.HBM)


def body(spectral_field, fwd, inv, last, counts):
    updated, spectrum = pl.pallas_call(
        transform_kernel,
        out_shape=(
            pltpu.VMEM((2, 8, 32, 256), F32),
            pltpu.VMEM((1, 256), F32),
        ),
        in_specs=[HBM] * 5,
        out_specs=(VMEM, VMEM),
        scratch_shapes=[
            pltpu.VMEM((2, 8, 32, 256), F32),
            pltpu.VMEM((512, 512), BF16),
            pltpu.VMEM((512, 512), BF16),
            pltpu.VMEM((1024, 512), BF16),
            pltpu.VMEM((1, 256), F32),
            pltpu.VMEM((512, 512), BF16),
            pltpu.VMEM((128, 128), BF16),
            pltpu.VMEM((1024, 1024), BF16),
            pltpu.VMEM((2, 4, 8, 2, 8, 256), BF16),
            pltpu.VMEM((2, 4, 8, 2, 8, 256), BF16),
            pltpu.VMEM((2, 8, 8, 256), BF16),
            pltpu.VMEM((2, 8, 4, 4, 2, 8, 128), BF16),
            pltpu.VMEM((2, 4, 8, 4, 2, 8, 128), BF16),
            pltpu.VMEM((2, 512, 256), BF16),
            pltpu.VMEM((2, 8, 4, 4, 2, 8, 128), BF16),
            pltpu.VMEM((2, 8, 4, 4, 2, 8, 128), BF16),
            pltpu.VMEM((2, 4, 8, 32, 128), BF16),
            pltpu.VMEM((2, 4, 8, 32, 128), BF16),
            pltpu.VMEM((2, 8, 32, 512), BF16),
            pltpu.VMEM((2, 256, 128), jnp.int32),
            pltpu.VMEM((1, 256), F32),
            pltpu.VMEM((32, 1, 256), F32),
            pltpu.VMEM((8, 1, 256), F32),
            pltpu.VMEM((1, 256), F32),
        ] + [pltpu.SemaphoreType.DMA((2, 4))] * 8 + [pltpu.SemaphoreType.DMA((5,))] + [
            pltpu.SemaphoreType.DMA((1,))] * 4,
        compiler_params=pltpu.CompilerParams(
            collective_id=0, has_side_effects=True, vmem_limit_bytes=50 * 1024 * 1024),
        name="transforms",
    )(*(pltpu.with_memory_space_constraint(x, pltpu.HBM) for x in (spectral_field, fwd, inv, last, counts)))
    return updated, spectrum.reshape(256)


def solution(mesh):
    consts = tables()
    step = functools.partial(jax.shard_map, mesh=mesh, check_vma=False)

    def run(spectral_field):
        return step(
            lambda f: body(f, *(jnp.asarray(c) for c in consts)),
            in_specs=(P(None, "row", "col", None),),
            out_specs=(P(None, "row", "col", None), P()),
        )(spectral_field)

    return run
```

```python
import functools
import math

import jax
import jax.numpy as jnp
import numpy as np
from jax import lax
from jax.experimental import pallas as pl
from jax.experimental.pallas import tpu as pltpu
from jax.sharding import PartitionSpec as P

PHASE_RATE = 0.0002
COUPLING = 0.2
K = 256
N = 512
BF16 = jnp.bfloat16
F32 = jnp.float32


def mm(a, b):
    return lax.dot_general(a, b, (((1,), (0,)), ((), ())), preferred_element_type=F32)


def mmt(a, b):
    return lax.dot_general(a, b, (((1,), (1,)), ((), ())), preferred_element_type=F32)


def iota(shape, dim):
    return lax.broadcasted_iota(jnp.int32, shape, dim)


def one_hot(hit):
    return jnp.where(hit, 1.0, 0.0).astype(BF16)


def shell_room(rad2, part):
    s = iota((1, 128), 1) + part * 128
    return s * s + s - rad2


def shell_reach(rad2, part):
    room = jnp.maximum(shell_room(rad2, part), 0).astype(F32)
    return jnp.minimum(jnp.sqrt(room + 0.5).astype(jnp.int32), 127)


def shell_sums(energy, rad2, reach):
    j = jnp.abs(iota((256, 128), 0) - 128)
    within = jnp.where(j <= iota((256, 128), 1), 1.0, 0.0)
    prefix = lax.dot_general(energy, within, (((1,), (0,)), ((), ())),
                             preferred_element_type=F32, precision=lax.Precision.HIGHEST)
    parts = []
    for part in range(2):
        room = shell_room(rad2, part)
        inner = jnp.take_along_axis(prefix, reach[part], axis=1, mode="promise_in_bounds")
        total = jnp.where(room >= 0, inner, 0.0) + jnp.where(room >= 128 * 128, energy[:, :1], 0.0)
        parts.append(jnp.sum(total, axis=0, keepdims=True))
    lane = iota((1, 256), 1)
    shifted = jnp.concatenate([pltpu.roll(parts[0], 1, 1), pltpu.roll(parts[1], 1, 1)], axis=1)
    shifted = jnp.where(lane == 0, 0.0, jnp.where(lane == 128, parts[0][:, 127:], shifted))
    return jnp.concatenate(parts, axis=1) - shifted


def transform_kernel(
    field_hbm, fwd_hbm, inv_hbm, last_hbm, counts_hbm, out, spectrum,
    field, fwd, inv, last, counts, p1, p2, p3, eye, aout, bin_, xr, bout, cin, yb, cub, xb, cout, din, dout, ein, zb, reach,
    shells, first, second, mid,
    s1, r1, s2, r2, s3, r3, s4, r4, load_sem, s5, r5, s6, r6,
):
    row = lax.axis_index("row")
    xh = lax.axis_index("col")
    zl = row // 8
    yc = row % 8

    def remote(src, dst, send, recv, to_row, to_col):
        return pltpu.make_async_remote_copy(
            src_ref=src, dst_ref=dst, send_sem=send, recv_sem=recv,
            device_id={"row": to_row, "col": to_col}, device_id_type=pl.DeviceIdType.MESH,
        )

    loads = [
        pltpu.make_async_copy(field_hbm, field, load_sem.at[0]),
        pltpu.make_async_copy(inv_hbm, inv, load_sem.at[1]),
        pltpu.make_async_copy(fwd_hbm, fwd, load_sem.at[2]),
        pltpu.make_async_copy(last_hbm, last, load_sem.at[3]),
        pltpu.make_async_copy(counts_hbm, counts, load_sem.at[4]),
    ]
    for load in loads:
        load.start()

    barrier = pltpu.get_barrier_semaphore()

    @pl.loop(1, 32)
    def _(i):
        d = (zl * 8 + xh + i) % 32
        pl.semaphore_signal(
            barrier, inc=1, device_id={"row": (d // 8) * 8 + yc, "col": d % 8},
            device_id_type=pl.DeviceIdType.MESH,
        )

    @pl.loop(1, 8)
    def _(j):
        pl.semaphore_signal(
            barrier, inc=1, device_id={"row": zl * 8 + (yc + j) % 8, "col": xh},
            device_id_type=pl.DeviceIdType.MESH,
        )

    def wait(ref, sem):
        pltpu.make_async_copy(ref, ref, sem).wait()

    def copy1(h, k, i):
        zd = (zl + 6 - k) % 4
        xd = (xh + i) % 8
        return remote(aout.at[h, zd, xd], bin_.at[h, zl, xh], s1.at[h, k], r1.at[h, k], zd * 8 + yc, xd)

    def copy2(h, k, j):
        zs = (zl + k + 2) % 4
        yd = (yc + j) % 8
        return remote(bout.at[h, yd, zs], cin.at[h, zs, yc], s2.at[h, k], r2.at[h, k], zl * 8 + yd, xh)

    def copy3(h, k, j):
        zs = (zl + k + 3) % 4
        yd = (yc + j) % 8
        return remote(cout.at[h, yd, zs], din.at[h, zs, yc], s3.at[h, k], r3.at[h, k], zl * 8 + yd, xh)

    def copy4(h, k, i):
        zd = (zl + k + 3) % 4
        xd = (xh + i) % 8
        return remote(dout.at[h, zd, xd], ein.at[h, zl, xh], s4.at[h, k], r4.at[h, k], zd * 8 + yc, xd)

    def start_all(copy, h, k, own):
        @pl.when(k != own)
        def _():
            copy(h, k, 0).start()

        @pl.loop(1, 8)
        def _(i):
            copy(h, k, i).start()

    def wait_all(ref, sem, h, k, own):
        @pl.when(k != own)
        def _():
            wait(ref.at[h, 0], sem.at[h, k])

        @pl.when(k == own)
        def _():
            wait(ref.at[h, 0, pl.ds(0, 7)], sem.at[h, k])

    me1 = zl * 8 + xh

    def copy5(i):
        d = (me1 + i) % 32
        return remote(shells, first.at[me1], s5.at[0], r5.at[0], (d // 8) * 8 + yc, d % 8)

    def copy6(j):
        return remote(mid, second.at[yc], s6.at[0], r6.at[0], zl * 8 + (yc + j) % 8, xh)

    j1 = iota((128, 512), 1)
    f1 = ((j1 // 32) % 4) * 128 + (j1 // 128) * 32 + j1 % 32

    @pl.loop(0, 4)
    def _(b):
        rows = pl.ds(pl.multiple_of(b * 128, 128), 128)
        p1[rows, :] = one_hot(iota((128, 512), 0) + b * 128 == f1)

    q2 = iota((128, 128), 0)
    p2[...] = one_hot(iota((128, 128), 1) == (q2 // 64) * 64 + (q2 % 8) * 8 + (q2 // 8) % 8)

    eye[...] = one_hot(iota((256, 256), 0) == iota((256, 256), 1))
    j3 = iota((128, 1024), 1)
    f3 = ((j3 // 8) % 8) * 128 + (j3 % 8) * 16 + ((j3 // 64) % 2) * 8 + j3 // 128

    @pl.loop(0, 8)
    def _(b):
        rows = pl.ds(pl.multiple_of(b * 128, 128), 128)
        p3[rows, :] = one_hot(iota((128, 1024), 0) + b * 128 == f3)

    loads[0].wait()
    loads[1].wait()

    @pl.loop(0, 4)
    def _(zd):
        rows = pl.ds(pl.multiple_of(zd * 128, 128), 128)
        c, s = inv[rows, :256], inv[rows, 256:]
        re = field[0].reshape(256, 256).astype(BF16)
        im = field[1].reshape(256, 256).astype(BF16)
        pair = (
            (mmt(c, re) - mmt(s, im)) * (1.0 / 16.0),
            (mmt(s, re) + mmt(c, im)) * (1.0 / 16.0),
        )
        for ri in range(2):
            v = pair[ri].reshape(8, 2, 8, 256)
            for h in range(2):
                aout[h, zd, :, ri] = v[:, h].astype(BF16)

    for h in range(2):
        bin_[h, zl, xh] = aout[h, zl, xh]
    pl.semaphore_wait(barrier, 38)

    @pl.loop(0, 2)
    def _(h):
        @pl.loop(0, 4)
        def _(k):
            start_all(copy1, h, k, 2)

    wz = iota((1, 256), 1) - 128
    r = iota((256, 1), 0)
    wx = row * 8 - 128 + r // 32
    wy = xh * 32 - 128 + r % 32
    rad2 = wx * wx + wy * wy
    for part in range(2):
        reach[part] = shell_reach(rad2, part)

    loads[2].wait()
    loads[3].wait()
    loads[4].wait()

    def stage_b(h, k):
        zs = (zl + k + 2) % 4
        parts = []
        for ht in range(2):
            for xt in range(2):
                lanes = slice(xt * 128, xt * 128 + 128)
                parts.append(jnp.concatenate(
                    [bin_[h, zs, ht * 4 + q, :, :, lanes].reshape(16, 128) for q in range(4)], axis=1))
        o = mm(jnp.concatenate(parts, axis=0), p1[...])
        for ht in range(2):
            for xt in range(2):
                base = (ht * 2 + xt) * 16
                for c in range(2):
                    for x in range(4):
                        xr[c, xt * 4 + x, :, ht * 128:ht * 128 + 128] = (
                            o[base + c * 8:base + c * 8 + 8, x * 128:x * 128 + 128].astype(BF16))
        q = mm(p2[...], xr[...].reshape(128, 256)).reshape(2, 8, 8, 256)
        for c in range(2):
            bout[h, :, zs, c] = q[c].astype(BF16)
        cin[h, zs, yc] = bout[h, yc, zs]

    @pl.loop(0, 2)
    def _(h):
        @pl.loop(0, 4)
        def _(k):
            wait_all(bin_, r1, h, k, 2)
            stage_b(h, k)

            @pl.loop(1, 8)
            def _(j):
                copy2(h, k, j).start()

    def plane_y(h):
        for half in range(2):
            d = jnp.concatenate(
                [cin[h, half * 2:half * 2 + 2, :, c].reshape(128, 256) for c in range(2)], axis=0)
            mc = mm(d, fwd[:256, :])
            ms = mm(d, fwd[256:, :])
            pair = ((mc[:128] - ms[128:]) * (1.0 / 16.0), (ms[:128] + mc[128:]) * (1.0 / 16.0))
            for c in range(2):
                for y in range(4):
                    yb[y, c, half * 128:half * 128 + 128, :] = pair[c][:, y * 128:y * 128 + 128].astype(BF16)

    def plane_x(y, slot):
        d = jnp.concatenate([yb[y, 0], yb[y, 1]], axis=1)
        d = jnp.concatenate([d, jnp.concatenate([-d[:, 128:], d[:, :128]], axis=1)], axis=0)
        for half in range(2):
            rows = slice(half * 256, half * 256 + 256)
            phys = mm(inv[rows, :], d) * (1.0 / 16.0)
            re, im = phys[:, :128], phys[:, 128:]
            gain = COUPLING * (re * re + im * im)
            cub[slot, rows, :128] = (gain * re).astype(BF16)
            cub[slot, rows, 128:] = (gain * im).astype(BF16)

    def plane_x_back(y, slot):
        m = mm(fwd[...], cub[slot])
        xb[y, 0] = ((m[:256, :128] + m[256:, 128:]) * (1.0 / 32.0)).astype(BF16)
        xb[y, 1] = ((m[:256, 128:] - m[256:, :128]) * (1.0 / 32.0)).astype(BF16)

    def plane_y_back(h):
        for half in range(2):
            rows = slice(half * 128, half * 128 + 128)
            d = jnp.concatenate(
                [jnp.concatenate([xb[y, c, rows, :] for y in range(4)], axis=1) for c in range(2)], axis=0)
            m = mm(d, inv[...])
            pair = (
                (m[:128, :256] + m[128:, 256:]) * (1.0 / 32.0),
                (m[128:, :256] - m[:128, 256:]) * (1.0 / 32.0),
            )
            for c in range(2):
                v = pair[c].reshape(2, 8, 8, 256)
                for q in range(2):
                    cout[h, :, half * 2 + q, c] = v[q].astype(BF16)

    @pl.loop(0, 2)
    def _(h):
        @pl.loop(0, 4)
        def _(k):
            wait(cin.at[h, 0, pl.ds(0, 7)], r2.at[h, k])

        plane_y(h)

        @pl.loop(0, 2)
        def _(y):
            plane_x(2 * y, 0)
            plane_x(2 * y + 1, 1)
            plane_x_back(2 * y, 0)
            plane_x_back(2 * y + 1, 1)

        plane_y_back(h)

        @pl.loop(0, 4)
        def _(k):
            @pl.loop(1, 8)
            def _(j):
                copy3(h, k, j).start()

        din[h, :, yc] = cout[h, yc]

    def stage_d(h, k):
        zs = (zl + k + 3) % 4
        o = mmt(eye[...], din[h, zs].reshape(128, 256))
        dout[h, zs] = o.astype(BF16).reshape(8, 32, 128)

    @pl.loop(0, 2)
    def _(h):
        @pl.loop(0, 4)
        def _(k):
            wait(din.at[h, 0, pl.ds(0, 7)], r3.at[h, k])
            stage_d(h, k)
            start_all(copy4, h, k, 1)

        ein[h, zl, xh] = dout[h, zl, xh]

    for h in range(2):
        @pl.loop(0, 4)
        def _(k, h=h):
            wait_all(ein, r4, h, k, 1)

        parts = [jnp.concatenate([ein[h, g, s] for s in range(8)], axis=1) for g in range(4)]
        o = mm(jnp.concatenate(parts, axis=0), p3[...]).astype(BF16)
        for g in range(4):
            for x in range(8):
                zb[h, x, :, g * 128:g * 128 + 128] = o[g * 32:g * 32 + 32, x * 128:x * 128 + 128]
        nl = mm(zb[h].reshape(256, 512), last[h * 512:h * 512 + 512, :]) * (1.0 / 32.0)
        base = field if h == 0 else out
        u = base[0].reshape(256, 256) - nl[:, 256:]
        v = base[1].reshape(256, 256) + nl[:, :256]
        out[0] = u.reshape(8, 32, 256)
        out[1] = v.reshape(8, 32, 256)

    shells[...] = shell_sums(u * u + v * v, rad2, reach)
    first[me1] = shells[...]

    @pl.loop(1, 32)
    def _(i):
        copy5(i).start()

    az = PHASE_RATE * (wz * wz).astype(F32)
    ar = PHASE_RATE * rad2.astype(F32)
    cz, sz = jnp.cos(az), jnp.sin(az)
    cr, sr = jnp.cos(ar), jnp.sin(ar)
    cos = (cr * cz - sr * sz).reshape(8, 32, 256)
    sin = (sr * cz + cr * sz).reshape(8, 32, 256)
    u, v = out[0], out[1]
    out[0] = u * cos + v * sin
    out[1] = v * cos - u * sin

    wait(first.at[pl.ds(0, 31)], r5.at[0])

    mid[...] = jnp.sum(first[...], axis=0)
    second[yc] = mid[...]

    @pl.loop(1, 8)
    def _(j):
        copy6(j).start()

    wait(second.at[pl.ds(0, 7)], r6.at[0])

    spectrum[...] = jnp.sum(second[...], axis=0) / counts[...]

    @pl.loop(0, 2)
    def _(h):
        @pl.loop(0, 4)
        def _(k):
            wait_all(aout, s1, h, k, 2)
            wait(bout.at[h, pl.ds(0, 7), 0], s2.at[h, k])
            wait(cout.at[h, pl.ds(0, 7), 0], s3.at[h, k])
            wait_all(dout, s4, h, k, 1)

    wait(first.at[pl.ds(0, 31)], s5.at[0])
    wait(second.at[pl.ds(0, 7)], s6.at[0])


def tables():
    waves = np.arange(K, dtype=np.int64) - K // 2
    phase = (waves[:, None] * np.arange(N, dtype=np.int64)[None, :]) % N
    angle = phase.astype(np.float32) * np.float32(2.0 * math.pi / N)
    cos = np.cos(angle).astype(jnp.bfloat16)
    sin = np.sin(angle).astype(jnp.bfloat16)
    fwd = np.concatenate([cos, sin], axis=0)
    inv = np.concatenate([cos.T, sin.T], axis=1)
    h, g, c, s, z = np.meshgrid(*(np.arange(n) for n in (2, 4, 2, 8, 8)), indexing="ij")
    point = ((g * 8 + s) * 16 + h * 8 + z).reshape(-1)
    is_re = (c.reshape(-1) == 0)[:, None]
    ct, st = cos.T[point], sin.T[point]
    last = np.concatenate([np.where(is_re, ct, st), np.where(is_re, -st, ct)], axis=1)
    sq = waves * waves
    q = (sq[:, None] + sq[None, :]).reshape(-1)
    pairs = np.bincount(q, minlength=2 * (K // 2) ** 2 + 1)
    counts = np.zeros(K, np.float64)
    radii = np.nonzero(pairs)[0]
    for w2 in sq:
        shell = np.floor(np.sqrt((radii + w2).astype(np.float64)) + 0.5).astype(np.int64)
        counts += np.bincount(shell, weights=pairs[radii], minlength=K)[:K]
    return fwd, np.ascontiguousarray(inv), last, np.maximum(counts, 1.0).astype(np.float32).reshape(1, K)


VMEM = pl.BlockSpec(memory_space=pltpu.VMEM)
HBM = pl.BlockSpec(memory_space=pltpu.HBM)


def body(spectral_field, fwd, inv, last, counts):
    updated, spectrum = pl.pallas_call(
        transform_kernel,
        out_shape=(
            pltpu.VMEM((2, 8, 32, 256), F32),
            pltpu.VMEM((1, 256), F32),
        ),
        in_specs=[HBM] * 5,
        out_specs=(VMEM, VMEM),
        scratch_shapes=[
            pltpu.VMEM((2, 8, 32, 256), F32),
            pltpu.VMEM((512, 512), BF16),
            pltpu.VMEM((512, 512), BF16),
            pltpu.VMEM((1024, 512), BF16),
            pltpu.VMEM((1, 256), F32),
            pltpu.VMEM((512, 512), BF16),
            pltpu.VMEM((128, 128), BF16),
            pltpu.VMEM((1024, 1024), BF16),
            pltpu.VMEM((256, 256), BF16),
            pltpu.VMEM((2, 4, 8, 2, 8, 256), BF16),
            pltpu.VMEM((2, 4, 8, 2, 8, 256), BF16),
            pltpu.VMEM((2, 8, 8, 256), BF16),
            pltpu.VMEM((2, 8, 4, 2, 8, 256), BF16),
            pltpu.VMEM((2, 4, 8, 2, 8, 256), BF16),
            pltpu.VMEM((4, 2, 256, 128), BF16),
            pltpu.VMEM((2, 512, 256), BF16),
            pltpu.VMEM((4, 2, 256, 128), BF16),
            pltpu.VMEM((2, 8, 4, 2, 8, 256), BF16),
            pltpu.VMEM((2, 4, 8, 2, 8, 256), BF16),
            pltpu.VMEM((2, 4, 8, 32, 128), BF16),
            pltpu.VMEM((2, 4, 8, 32, 128), BF16),
            pltpu.VMEM((2, 8, 32, 512), BF16),
            pltpu.VMEM((2, 256, 128), jnp.int32),
            pltpu.VMEM((1, 256), F32),
            pltpu.VMEM((32, 1, 256), F32),
            pltpu.VMEM((8, 1, 256), F32),
            pltpu.VMEM((1, 256), F32),
        ] + [pltpu.SemaphoreType.DMA((2, 4))] * 8 + [pltpu.SemaphoreType.DMA((5,))] + [
            pltpu.SemaphoreType.DMA((1,))] * 4,
        compiler_params=pltpu.CompilerParams(
            collective_id=0, has_side_effects=True, vmem_limit_bytes=50 * 1024 * 1024),
        name="transforms",
    )(*(pltpu.with_memory_space_constraint(x, pltpu.HBM) for x in (spectral_field, fwd, inv, last, counts)))
    return updated, spectrum.reshape(256)


def solution(mesh):
    consts = tables()
    step = functools.partial(jax.shard_map, mesh=mesh, check_vma=False)

    def run(spectral_field):
        return step(
            lambda f: body(f, *(jnp.asarray(c) for c in consts)),
            in_specs=(P(None, "row", "col", None),),
            out_specs=(P(None, "row", "col", None), P()),
        )(spectral_field)

    return run
```

```python
import functools
import math

import jax
import jax.numpy as jnp
import numpy as np
from jax import lax
from jax.experimental import pallas as pl
from jax.experimental.pallas import tpu as pltpu
from jax.sharding import PartitionSpec as P

PHASE_RATE = 0.0002
COUPLING = 0.2
K = 256
N = 512
BF16 = jnp.bfloat16
F32 = jnp.float32


def mm(a, b):
    return lax.dot_general(a, b, (((1,), (0,)), ((), ())), preferred_element_type=F32)


def mmt(a, b):
    return lax.dot_general(a, b, (((1,), (1,)), ((), ())), preferred_element_type=F32)


def iota(shape, dim):
    return lax.broadcasted_iota(jnp.int32, shape, dim)


def one_hot(hit):
    return jnp.where(hit, 1.0, 0.0).astype(BF16)


def shell_room(rad2, part):
    s = iota((1, 128), 1) + part * 128
    return s * s + s - rad2


def shell_reach(rad2, part):
    room = jnp.maximum(shell_room(rad2, part), 0).astype(F32)
    return jnp.minimum(jnp.sqrt(room + 0.5).astype(jnp.int32), 127)


def shell_sums(energy, rad2, reach):
    j = jnp.abs(iota((256, 128), 0) - 128)
    within = jnp.where(j <= iota((256, 128), 1), 1.0, 0.0)
    prefix = lax.dot_general(energy, within, (((1,), (0,)), ((), ())),
                             preferred_element_type=F32, precision=lax.Precision.HIGHEST)
    parts = []
    for part in range(2):
        room = shell_room(rad2, part)
        inner = jnp.take_along_axis(prefix, reach[part], axis=1, mode="promise_in_bounds")
        total = jnp.where(room >= 0, inner, 0.0) + jnp.where(room >= 128 * 128, energy[:, :1], 0.0)
        parts.append(jnp.sum(total, axis=0, keepdims=True))
    lane = iota((1, 256), 1)
    shifted = jnp.concatenate([pltpu.roll(parts[0], 1, 1), pltpu.roll(parts[1], 1, 1)], axis=1)
    shifted = jnp.where(lane == 0, 0.0, jnp.where(lane == 128, parts[0][:, 127:], shifted))
    return jnp.concatenate(parts, axis=1) - shifted


def transform_kernel(
    field_hbm, fwd_hbm, inv_hbm, last_hbm, counts_hbm, out, spectrum,
    field, fwd, inv, last, counts, p1, p2, p3, eye, aout, bin_, xr, bout, cin, yb, cub, xb, cout, din, dout, ein, zb, reach,
    shells, first, second, mid,
    s1, r1, s2, r2, s3, r3, s4, r4, load_sem, s5, r5, s6, r6,
):
    row = lax.axis_index("row")
    xh = lax.axis_index("col")
    zl = row // 8
    yc = row % 8

    def remote(src, dst, send, recv, to_row, to_col):
        return pltpu.make_async_remote_copy(
            src_ref=src, dst_ref=dst, send_sem=send, recv_sem=recv,
            device_id={"row": to_row, "col": to_col}, device_id_type=pl.DeviceIdType.MESH,
        )

    loads = [
        pltpu.make_async_copy(field_hbm, field, load_sem.at[0]),
        pltpu.make_async_copy(inv_hbm, inv, load_sem.at[1]),
        pltpu.make_async_copy(fwd_hbm, fwd, load_sem.at[2]),
        pltpu.make_async_copy(last_hbm, last, load_sem.at[3]),
        pltpu.make_async_copy(counts_hbm, counts, load_sem.at[4]),
    ]
    for load in loads[:2]:
        load.start()

    barrier = pltpu.get_barrier_semaphore()

    @pl.loop(1, 32)
    def _(i):
        d = (zl * 8 + xh + i) % 32
        pl.semaphore_signal(
            barrier, inc=1, device_id={"row": (d // 8) * 8 + yc, "col": d % 8},
            device_id_type=pl.DeviceIdType.MESH,
        )

    @pl.loop(1, 8)
    def _(j):
        pl.semaphore_signal(
            barrier, inc=1, device_id={"row": zl * 8 + (yc + j) % 8, "col": xh},
            device_id_type=pl.DeviceIdType.MESH,
        )

    def wait(ref, sem):
        pltpu.make_async_copy(ref, ref, sem).wait()

    def copy1(h, k, i):
        zd = (zl + 6 - k) % 4
        xd = (xh + i) % 8
        return remote(aout.at[h, zd, xd], bin_.at[h, zl, xh], s1.at[h, k], r1.at[h, k], zd * 8 + yc, xd)

    def copy2(h, k, j):
        zs = (zl + k + 2) % 4
        yd = (yc + j) % 8
        return remote(bout.at[h, yd, zs], cin.at[h, zs, yc], s2.at[h, k], r2.at[h, k], zl * 8 + yd, xh)

    def copy3(h, k, j):
        zs = (zl + k + 3) % 4
        yd = (yc + j) % 8
        return remote(cout.at[h, yd, zs], din.at[h, zs, yc], s3.at[h, k], r3.at[h, k], zl * 8 + yd, xh)

    def copy4(h, k, i):
        zd = (zl + k + 3) % 4
        xd = (xh + i) % 8
        return remote(dout.at[h, zd, xd], ein.at[h, zl, xh], s4.at[h, k], r4.at[h, k], zd * 8 + yc, xd)

    def start_all(copy, h, k, own):
        @pl.when(jnp.asarray(k) != own)
        def _():
            copy(h, k, 0).start()

        @pl.loop(1, 8)
        def _(i):
            copy(h, k, i).start()

    def wait_all(ref, sem, h, k, own):
        @pl.when(k != own)
        def _():
            wait(ref.at[h, 0], sem.at[h, k])

        @pl.when(k == own)
        def _():
            wait(ref.at[h, 0, pl.ds(0, 7)], sem.at[h, k])

    me1 = zl * 8 + xh

    def copy5(i):
        d = (me1 + i) % 32
        return remote(shells, first.at[me1], s5.at[0], r5.at[0], (d // 8) * 8 + yc, d % 8)

    def copy6(j):
        return remote(mid, second.at[yc], s6.at[0], r6.at[0], zl * 8 + (yc + j) % 8, xh)

    for load in loads[2:]:
        load.start()
    loads[0].wait()
    loads[1].wait()

    def stage_a(k):
        zd = (zl + 6 - k) % 4
        rows = pl.ds(pl.multiple_of(zd * 128, 128), 128)
        c, s = inv[rows, :256], inv[rows, 256:]
        re = field[0].reshape(256, 256).astype(BF16)
        im = field[1].reshape(256, 256).astype(BF16)
        pair = (
            (mmt(c, re) - mmt(s, im)) * (1.0 / 16.0),
            (mmt(s, re) + mmt(c, im)) * (1.0 / 16.0),
        )
        for ri in range(2):
            v = pair[ri].reshape(8, 2, 8, 256)
            for h in range(2):
                aout[h, zd, :, ri] = v[:, h].astype(BF16)

    stage_a(0)
    pl.semaphore_wait(barrier, 38)
    start_all(copy1, 0, 0, 2)

    @pl.loop(1, 4)
    def _(k):
        stage_a(k)
        start_all(copy1, 0, k, 2)

    @pl.loop(0, 4)
    def _(k):
        start_all(copy1, 1, k, 2)

    for h in range(2):
        bin_[h, zl, xh] = aout[h, zl, xh]

    j1 = iota((128, 512), 1)
    f1 = ((j1 // 32) % 4) * 128 + (j1 // 128) * 32 + j1 % 32

    @pl.loop(0, 4)
    def _(b):
        rows = pl.ds(pl.multiple_of(b * 128, 128), 128)
        p1[rows, :] = one_hot(iota((128, 512), 0) + b * 128 == f1)

    q2 = iota((128, 128), 0)
    p2[...] = one_hot(iota((128, 128), 1) == (q2 // 64) * 64 + (q2 % 8) * 8 + (q2 // 8) % 8)

    eye[...] = one_hot(iota((256, 256), 0) == iota((256, 256), 1))
    j3 = iota((128, 1024), 1)
    f3 = ((j3 // 8) % 8) * 128 + (j3 % 8) * 16 + ((j3 // 64) % 2) * 8 + j3 // 128

    @pl.loop(0, 8)
    def _(b):
        rows = pl.ds(pl.multiple_of(b * 128, 128), 128)
        p3[rows, :] = one_hot(iota((128, 1024), 0) + b * 128 == f3)

    wz = iota((1, 256), 1) - 128
    r = iota((256, 1), 0)
    wx = row * 8 - 128 + r // 32
    wy = xh * 32 - 128 + r % 32
    rad2 = wx * wx + wy * wy
    for part in range(2):
        reach[part] = shell_reach(rad2, part)

    loads[2].wait()
    loads[3].wait()
    loads[4].wait()

    def stage_b(h, k):
        zs = (zl + k + 2) % 4
        parts = []
        for ht in range(2):
            for xt in range(2):
                lanes = slice(xt * 128, xt * 128 + 128)
                parts.append(jnp.concatenate(
                    [bin_[h, zs, ht * 4 + q, :, :, lanes].reshape(16, 128) for q in range(4)], axis=1))
        o = mm(jnp.concatenate(parts, axis=0), p1[...])
        for ht in range(2):
            for xt in range(2):
                base = (ht * 2 + xt) * 16
                for c in range(2):
                    for x in range(4):
                        xr[c, xt * 4 + x, :, ht * 128:ht * 128 + 128] = (
                            o[base + c * 8:base + c * 8 + 8, x * 128:x * 128 + 128].astype(BF16))
        q = mm(p2[...], xr[...].reshape(128, 256)).reshape(2, 8, 8, 256)
        for c in range(2):
            bout[h, :, zs, c] = q[c].astype(BF16)
        cin[h, zs, yc] = bout[h, yc, zs]

    @pl.loop(0, 2)
    def _(h):
        @pl.loop(0, 4)
        def _(k):
            wait_all(bin_, r1, h, k, 2)
            stage_b(h, k)

            @pl.loop(1, 8)
            def _(j):
                copy2(h, k, j).start()

    def plane_y(h):
        for half in range(2):
            d = jnp.concatenate(
                [cin[h, half * 2:half * 2 + 2, :, c].reshape(128, 256) for c in range(2)], axis=0)
            mc = mm(d, fwd[:256, :])
            ms = mm(d, fwd[256:, :])
            pair = ((mc[:128] - ms[128:]) * (1.0 / 16.0), (ms[:128] + mc[128:]) * (1.0 / 16.0))
            for c in range(2):
                for y in range(4):
                    yb[y, c, half * 128:half * 128 + 128, :] = pair[c][:, y * 128:y * 128 + 128].astype(BF16)

    def plane_x(y, slot):
        d = jnp.concatenate([yb[y, 0], yb[y, 1]], axis=1)
        d = jnp.concatenate([d, jnp.concatenate([-d[:, 128:], d[:, :128]], axis=1)], axis=0)
        for half in range(2):
            rows = slice(half * 256, half * 256 + 256)
            phys = mm(inv[rows, :], d) * (1.0 / 16.0)
            re, im = phys[:, :128], phys[:, 128:]
            gain = COUPLING * (re * re + im * im)
            cub[slot, rows, :128] = (gain * re).astype(BF16)
            cub[slot, rows, 128:] = (gain * im).astype(BF16)

    def plane_x_back(y, slot):
        m = mm(fwd[...], cub[slot])
        xb[y, 0] = ((m[:256, :128] + m[256:, 128:]) * (1.0 / 32.0)).astype(BF16)
        xb[y, 1] = ((m[:256, 128:] - m[256:, :128]) * (1.0 / 32.0)).astype(BF16)

    def plane_y_back(h):
        for half in range(2):
            rows = slice(half * 128, half * 128 + 128)
            d = jnp.concatenate(
                [jnp.concatenate([xb[y, c, rows, :] for y in range(4)], axis=1) for c in range(2)], axis=0)
            m = mm(d, inv[...])
            pair = (
                (m[:128, :256] + m[128:, 256:]) * (1.0 / 32.0),
                (m[128:, :256] - m[:128, 256:]) * (1.0 / 32.0),
            )
            for c in range(2):
                v = pair[c].reshape(2, 8, 8, 256)
                for q in range(2):
                    cout[h, :, half * 2 + q, c] = v[q].astype(BF16)

    @pl.loop(0, 2)
    def _(h):
        @pl.loop(0, 4)
        def _(k):
            wait(cin.at[h, 0, pl.ds(0, 7)], r2.at[h, k])

        plane_y(h)

        @pl.loop(0, 2)
        def _(y):
            plane_x(2 * y, 0)
            plane_x(2 * y + 1, 1)
            plane_x_back(2 * y, 0)
            plane_x_back(2 * y + 1, 1)

        plane_y_back(h)

        @pl.loop(0, 4)
        def _(k):
            @pl.loop(1, 8)
            def _(j):
                copy3(h, k, j).start()

        din[h, :, yc] = cout[h, yc]

    def stage_d(h, k):
        zs = (zl + k + 3) % 4
        o = mmt(eye[...], din[h, zs].reshape(128, 256))
        dout[h, zs] = o.astype(BF16).reshape(8, 32, 128)

    @pl.loop(0, 2)
    def _(h):
        @pl.loop(0, 4)
        def _(k):
            wait(din.at[h, 0, pl.ds(0, 7)], r3.at[h, k])
            stage_d(h, k)
            start_all(copy4, h, k, 1)

        ein[h, zl, xh] = dout[h, zl, xh]

    for h in range(2):
        @pl.loop(0, 4)
        def _(k, h=h):
            wait_all(ein, r4, h, k, 1)

        parts = [jnp.concatenate([ein[h, g, s] for s in range(8)], axis=1) for g in range(4)]
        o = mm(jnp.concatenate(parts, axis=0), p3[...]).astype(BF16)
        for g in range(4):
            for x in range(8):
                zb[h, x, :, g * 128:g * 128 + 128] = o[g * 32:g * 32 + 32, x * 128:x * 128 + 128]
        nl = mm(zb[h].reshape(256, 512), last[h * 512:h * 512 + 512, :]) * (1.0 / 32.0)
        base = field if h == 0 else out
        u = base[0].reshape(256, 256) - nl[:, 256:]
        v = base[1].reshape(256, 256) + nl[:, :256]
        out[0] = u.reshape(8, 32, 256)
        out[1] = v.reshape(8, 32, 256)

    shells[...] = shell_sums(u * u + v * v, rad2, reach)
    first[me1] = shells[...]

    @pl.loop(1, 32)
    def _(i):
        copy5(i).start()

    az = PHASE_RATE * (wz * wz).astype(F32)
    ar = PHASE_RATE * rad2.astype(F32)
    cz, sz = jnp.cos(az), jnp.sin(az)
    cr, sr = jnp.cos(ar), jnp.sin(ar)
    cos = (cr * cz - sr * sz).reshape(8, 32, 256)
    sin = (sr * cz + cr * sz).reshape(8, 32, 256)
    u, v = out[0], out[1]
    out[0] = u * cos + v * sin
    out[1] = v * cos - u * sin

    wait(first.at[pl.ds(0, 31)], r5.at[0])

    mid[...] = jnp.sum(first[...], axis=0)
    second[yc] = mid[...]

    @pl.loop(1, 8)
    def _(j):
        copy6(j).start()

    wait(second.at[pl.ds(0, 7)], r6.at[0])

    spectrum[...] = jnp.sum(second[...], axis=0) / counts[...]

    @pl.loop(0, 2)
    def _(h):
        @pl.loop(0, 4)
        def _(k):
            wait_all(aout, s1, h, k, 2)
            wait(bout.at[h, pl.ds(0, 7), 0], s2.at[h, k])
            wait(cout.at[h, pl.ds(0, 7), 0], s3.at[h, k])
            wait_all(dout, s4, h, k, 1)

    wait(first.at[pl.ds(0, 31)], s5.at[0])
    wait(second.at[pl.ds(0, 7)], s6.at[0])


def tables():
    waves = np.arange(K, dtype=np.int64) - K // 2
    phase = (waves[:, None] * np.arange(N, dtype=np.int64)[None, :]) % N
    angle = phase.astype(np.float32) * np.float32(2.0 * math.pi / N)
    cos = np.cos(angle).astype(jnp.bfloat16)
    sin = np.sin(angle).astype(jnp.bfloat16)
    fwd = np.concatenate([cos, sin], axis=0)
    inv = np.concatenate([cos.T, sin.T], axis=1)
    h, g, c, s, z = np.meshgrid(*(np.arange(n) for n in (2, 4, 2, 8, 8)), indexing="ij")
    point = ((g * 8 + s) * 16 + h * 8 + z).reshape(-1)
    is_re = (c.reshape(-1) == 0)[:, None]
    ct, st = cos.T[point], sin.T[point]
    last = np.concatenate([np.where(is_re, ct, st), np.where(is_re, -st, ct)], axis=1)
    sq = waves * waves
    q = (sq[:, None] + sq[None, :]).reshape(-1)
    pairs = np.bincount(q, minlength=2 * (K // 2) ** 2 + 1)
    counts = np.zeros(K, np.float64)
    radii = np.nonzero(pairs)[0]
    for w2 in sq:
        shell = np.floor(np.sqrt((radii + w2).astype(np.float64)) + 0.5).astype(np.int64)
        counts += np.bincount(shell, weights=pairs[radii], minlength=K)[:K]
    return fwd, np.ascontiguousarray(inv), last, np.maximum(counts, 1.0).astype(np.float32).reshape(1, K)


VMEM = pl.BlockSpec(memory_space=pltpu.VMEM)
HBM = pl.BlockSpec(memory_space=pltpu.HBM)


def body(spectral_field, fwd, inv, last, counts):
    updated, spectrum = pl.pallas_call(
        transform_kernel,
        out_shape=(
            pltpu.VMEM((2, 8, 32, 256), F32),
            pltpu.VMEM((1, 256), F32),
        ),
        in_specs=[HBM] * 5,
        out_specs=(VMEM, VMEM),
        scratch_shapes=[
            pltpu.VMEM((2, 8, 32, 256), F32),
            pltpu.VMEM((512, 512), BF16),
            pltpu.VMEM((512, 512), BF16),
            pltpu.VMEM((1024, 512), BF16),
            pltpu.VMEM((1, 256), F32),
            pltpu.VMEM((512, 512), BF16),
            pltpu.VMEM((128, 128), BF16),
            pltpu.VMEM((1024, 1024), BF16),
            pltpu.VMEM((256, 256), BF16),
            pltpu.VMEM((2, 4, 8, 2, 8, 256), BF16),
            pltpu.VMEM((2, 4, 8, 2, 8, 256), BF16),
            pltpu.VMEM((2, 8, 8, 256), BF16),
            pltpu.VMEM((2, 8, 4, 2, 8, 256), BF16),
            pltpu.VMEM((2, 4, 8, 2, 8, 256), BF16),
            pltpu.VMEM((4, 2, 256, 128), BF16),
            pltpu.VMEM((2, 512, 256), BF16),
            pltpu.VMEM((4, 2, 256, 128), BF16),
            pltpu.VMEM((2, 8, 4, 2, 8, 256), BF16),
            pltpu.VMEM((2, 4, 8, 2, 8, 256), BF16),
            pltpu.VMEM((2, 4, 8, 32, 128), BF16),
            pltpu.VMEM((2, 4, 8, 32, 128), BF16),
            pltpu.VMEM((2, 8, 32, 512), BF16),
            pltpu.VMEM((2, 256, 128), jnp.int32),
            pltpu.VMEM((1, 256), F32),
            pltpu.VMEM((32, 1, 256), F32),
            pltpu.VMEM((8, 1, 256), F32),
            pltpu.VMEM((1, 256), F32),
        ] + [pltpu.SemaphoreType.DMA((2, 4))] * 8 + [pltpu.SemaphoreType.DMA((5,))] + [
            pltpu.SemaphoreType.DMA((1,))] * 4,
        compiler_params=pltpu.CompilerParams(
            collective_id=0, has_side_effects=True, vmem_limit_bytes=50 * 1024 * 1024),
        name="transforms",
    )(*(pltpu.with_memory_space_constraint(x, pltpu.HBM) for x in (spectral_field, fwd, inv, last, counts)))
    return updated, spectrum.reshape(256)


def solution(mesh):
    consts = tables()
    step = functools.partial(jax.shard_map, mesh=mesh, check_vma=False)

    def run(spectral_field):
        return step(
            lambda f: body(f, *(jnp.asarray(c) for c in consts)),
            in_specs=(P(None, "row", "col", None),),
            out_specs=(P(None, "row", "col", None), P()),
        )(spectral_field)

    return run
```

```python
import functools
import math

import jax
import jax.numpy as jnp
import numpy as np
from jax import lax
from jax.experimental import pallas as pl
from jax.experimental.pallas import tpu as pltpu
from jax.sharding import PartitionSpec as P

PHASE_RATE = 0.0002
COUPLING = 0.2
K = 256
N = 512
BF16 = jnp.bfloat16
F32 = jnp.float32


def mm(a, b):
    return lax.dot_general(a, b, (((1,), (0,)), ((), ())), preferred_element_type=F32)


def mmt(a, b):
    return lax.dot_general(a, b, (((1,), (1,)), ((), ())), preferred_element_type=F32)


def iota(shape, dim):
    return lax.broadcasted_iota(jnp.int32, shape, dim)


def one_hot(hit):
    return jnp.where(hit, 1.0, 0.0).astype(BF16)


def shell_room(rad2, part):
    s = iota((1, 128), 1) + part * 128
    return s * s + s - rad2


def shell_reach(rad2, part):
    room = jnp.maximum(shell_room(rad2, part), 0).astype(F32)
    return jnp.minimum(jnp.sqrt(room + 0.5).astype(jnp.int32), 127)


def shell_sums(energy, rad2, reach):
    j = jnp.abs(iota((256, 128), 0) - 128)
    within = jnp.where(j <= iota((256, 128), 1), 1.0, 0.0)
    prefix = lax.dot_general(energy, within, (((1,), (0,)), ((), ())),
                             preferred_element_type=F32, precision=lax.Precision.HIGHEST)
    parts = []
    for part in range(2):
        room = shell_room(rad2, part)
        inner = jnp.take_along_axis(prefix, reach[part], axis=1, mode="promise_in_bounds")
        total = jnp.where(room >= 0, inner, 0.0) + jnp.where(room >= 128 * 128, energy[:, :1], 0.0)
        parts.append(jnp.sum(total, axis=0, keepdims=True))
    lane = iota((1, 256), 1)
    shifted = jnp.concatenate([pltpu.roll(parts[0], 1, 1), pltpu.roll(parts[1], 1, 1)], axis=1)
    shifted = jnp.where(lane == 0, 0.0, jnp.where(lane == 128, parts[0][:, 127:], shifted))
    return jnp.concatenate(parts, axis=1) - shifted


def transform_kernel(
    field_hbm, fwd_hbm, inv_hbm, last_hbm, counts_hbm, out, spectrum,
    field, fwd, inv, last, counts, p1, p2, p3, eye, aout, bin_, xr, bout, cin, yb, cub, xb, cout, din, dout, ein, zb, reach,
    shells, first, second, mid,
    s1, r1, s2, r2, s3, r3, s4, r4, load_sem, s5, r5, s6, r6,
):
    row = lax.axis_index("row")
    xh = lax.axis_index("col")
    zl = row // 8
    yc = row % 8

    def remote(src, dst, send, recv, to_row, to_col):
        return pltpu.make_async_remote_copy(
            src_ref=src, dst_ref=dst, send_sem=send, recv_sem=recv,
            device_id={"row": to_row, "col": to_col}, device_id_type=pl.DeviceIdType.MESH,
        )

    loads = [
        pltpu.make_async_copy(field_hbm, field, load_sem.at[0]),
        pltpu.make_async_copy(inv_hbm, inv, load_sem.at[1]),
        pltpu.make_async_copy(fwd_hbm, fwd, load_sem.at[2]),
        pltpu.make_async_copy(last_hbm, last, load_sem.at[3]),
        pltpu.make_async_copy(counts_hbm, counts, load_sem.at[4]),
    ]
    for load in loads[:2]:
        load.start()

    barrier = pltpu.get_barrier_semaphore()

    @pl.loop(1, 32)
    def _(i):
        d = (zl * 8 + xh + i) % 32
        pl.semaphore_signal(
            barrier, inc=1, device_id={"row": (d // 8) * 8 + yc, "col": d % 8},
            device_id_type=pl.DeviceIdType.MESH,
        )

    @pl.loop(1, 8)
    def _(j):
        pl.semaphore_signal(
            barrier, inc=1, device_id={"row": zl * 8 + (yc + j) % 8, "col": xh},
            device_id_type=pl.DeviceIdType.MESH,
        )

    def wait(ref, sem):
        pltpu.make_async_copy(ref, ref, sem).wait()

    def copy1(h, k, i):
        zd = (zl + 6 - k) % 4
        xd = (xh + i) % 8
        return remote(aout.at[h, zd, xd], bin_.at[h, zl, xh], s1.at[h, k], r1.at[h, k], zd * 8 + yc, xd)

    def copy2(h, k, j):
        zs = (zl + k + 2) % 4
        yd = (yc + j) % 8
        return remote(bout.at[h, yd, zs], cin.at[h, zs, yc], s2.at[h, k], r2.at[h, k], zl * 8 + yd, xh)

    def copy3(h, k, j):
        zs = (zl + k + 3) % 4
        yd = (yc + j) % 8
        return remote(cout.at[h, yd, zs], din.at[h, zs, yc], s3.at[h, k], r3.at[h, k], zl * 8 + yd, xh)

    def copy4(h, k, i):
        zd = (zl + k + 3) % 4
        xd = (xh + i) % 8
        return remote(dout.at[h, zd, xd], ein.at[h, zl, xh], s4.at[h, k], r4.at[h, k], zd * 8 + yc, xd)

    def start_all(copy, h, k, own):
        @pl.when(jnp.asarray(k) != own)
        def _():
            copy(h, k, 0).start()

        @pl.loop(1, 8)
        def _(i):
            copy(h, k, i).start()

    def wait_all(ref, sem, h, k, own):
        @pl.when(k != own)
        def _():
            wait(ref.at[h, 0], sem.at[h, k])

        @pl.when(k == own)
        def _():
            wait(ref.at[h, 0, pl.ds(0, 7)], sem.at[h, k])

    xc, z_hi, yy, core = xh // 2, xh % 2, yc // 2, yc % 2
    me1 = xc * 4 + yy
    me2 = (z_hi * 4 + zl) * 2 + core

    def copy5(i):
        d = (me1 + i) % 16
        return remote(shells, first.at[me1], s5.at[0], r5.at[0], zl * 8 + (d % 4) * 2 + core, (d // 4) * 2 + z_hi)

    def copy6(i):
        d = (me2 + i) % 16
        return remote(
            mid, second.at[me2], s6.at[0], r6.at[0], ((d // 2) % 4) * 8 + yy * 2 + d % 2, xc * 2 + d // 8)

    for load in loads[2:]:
        load.start()
    loads[0].wait()
    loads[1].wait()

    def stage_a(k):
        zd = (zl + 6 - k) % 4
        rows = pl.ds(pl.multiple_of(zd * 128, 128), 128)
        c, s = inv[rows, :256], inv[rows, 256:]
        re = field[0].reshape(256, 256).astype(BF16)
        im = field[1].reshape(256, 256).astype(BF16)
        pair = (
            (mmt(c, re) - mmt(s, im)) * (1.0 / 16.0),
            (mmt(s, re) + mmt(c, im)) * (1.0 / 16.0),
        )
        for ri in range(2):
            v = pair[ri].reshape(8, 2, 8, 256)
            for h in range(2):
                aout[h, zd, :, ri] = v[:, h].astype(BF16)

    stage_a(0)
    pl.semaphore_wait(barrier, 38)
    start_all(copy1, 0, 0, 2)

    @pl.loop(1, 4)
    def _(k):
        stage_a(k)
        start_all(copy1, 0, k, 2)

    @pl.loop(0, 4)
    def _(k):
        start_all(copy1, 1, k, 2)

    for h in range(2):
        bin_[h, zl, xh] = aout[h, zl, xh]

    j1 = iota((128, 512), 1)
    f1 = ((j1 // 32) % 4) * 128 + (j1 // 128) * 32 + j1 % 32

    @pl.loop(0, 4)
    def _(b):
        rows = pl.ds(pl.multiple_of(b * 128, 128), 128)
        p1[rows, :] = one_hot(iota((128, 512), 0) + b * 128 == f1)

    q2 = iota((128, 128), 0)
    p2[...] = one_hot(iota((128, 128), 1) == (q2 // 64) * 64 + (q2 % 8) * 8 + (q2 // 8) % 8)

    eye[...] = one_hot(iota((256, 256), 0) == iota((256, 256), 1))
    j3 = iota((128, 1024), 1)
    f3 = ((j3 // 8) % 8) * 128 + (j3 % 8) * 16 + ((j3 // 64) % 2) * 8 + j3 // 128

    @pl.loop(0, 8)
    def _(b):
        rows = pl.ds(pl.multiple_of(b * 128, 128), 128)
        p3[rows, :] = one_hot(iota((128, 1024), 0) + b * 128 == f3)

    wz = iota((1, 256), 1) - 128
    r = iota((256, 1), 0)
    wx = row * 8 - 128 + r // 32
    wy = xh * 32 - 128 + r % 32
    rad2 = wx * wx + wy * wy
    for part in range(2):
        reach[part] = shell_reach(rad2, part)

    loads[2].wait()
    loads[3].wait()
    loads[4].wait()

    def stage_b(h, k):
        zs = (zl + k + 2) % 4
        parts = []
        for ht in range(2):
            for xt in range(2):
                lanes = slice(xt * 128, xt * 128 + 128)
                parts.append(jnp.concatenate(
                    [bin_[h, zs, ht * 4 + q, :, :, lanes].reshape(16, 128) for q in range(4)], axis=1))
        o = mm(jnp.concatenate(parts, axis=0), p1[...])
        for ht in range(2):
            for xt in range(2):
                base = (ht * 2 + xt) * 16
                for c in range(2):
                    for x in range(4):
                        xr[c, xt * 4 + x, :, ht * 128:ht * 128 + 128] = (
                            o[base + c * 8:base + c * 8 + 8, x * 128:x * 128 + 128].astype(BF16))
        q = mm(p2[...], xr[...].reshape(128, 256)).reshape(2, 8, 8, 256)
        for c in range(2):
            bout[h, :, zs, c] = q[c].astype(BF16)
        cin[h, zs, yc] = bout[h, yc, zs]

    @pl.loop(0, 2)
    def _(h):
        @pl.loop(0, 4)
        def _(k):
            wait_all(bin_, r1, h, k, 2)
            stage_b(h, k)

            @pl.loop(1, 8)
            def _(j):
                copy2(h, k, j).start()

    def plane_y(h):
        for half in range(2):
            d = jnp.concatenate(
                [cin[h, half * 2:half * 2 + 2, :, c].reshape(128, 256) for c in range(2)], axis=0)
            mc = mm(d, fwd[:256, :])
            ms = mm(d, fwd[256:, :])
            pair = ((mc[:128] - ms[128:]) * (1.0 / 16.0), (ms[:128] + mc[128:]) * (1.0 / 16.0))
            for c in range(2):
                for y in range(4):
                    yb[y, c, half * 128:half * 128 + 128, :] = pair[c][:, y * 128:y * 128 + 128].astype(BF16)

    def plane_x(y, slot):
        d = jnp.concatenate([yb[y, 0], yb[y, 1]], axis=1)
        d = jnp.concatenate([d, jnp.concatenate([-d[:, 128:], d[:, :128]], axis=1)], axis=0)
        for half in range(2):
            rows = slice(half * 256, half * 256 + 256)
            phys = mm(inv[rows, :], d) * (1.0 / 16.0)
            re, im = phys[:, :128], phys[:, 128:]
            gain = COUPLING * (re * re + im * im)
            cub[slot, rows, :128] = (gain * re).astype(BF16)
            cub[slot, rows, 128:] = (gain * im).astype(BF16)

    def plane_x_back(y, slot):
        m = mm(fwd[...], cub[slot])
        xb[y, 0] = ((m[:256, :128] + m[256:, 128:]) * (1.0 / 32.0)).astype(BF16)
        xb[y, 1] = ((m[:256, 128:] - m[256:, :128]) * (1.0 / 32.0)).astype(BF16)

    def plane_y_back(h):
        for half in range(2):
            rows = slice(half * 128, half * 128 + 128)
            d = jnp.concatenate(
                [jnp.concatenate([xb[y, c, rows, :] for y in range(4)], axis=1) for c in range(2)], axis=0)
            m = mm(d, inv[...])
            pair = (
                (m[:128, :256] + m[128:, 256:]) * (1.0 / 32.0),
                (m[128:, :256] - m[:128, 256:]) * (1.0 / 32.0),
            )
            for c in range(2):
                v = pair[c].reshape(2, 8, 8, 256)
                for q in range(2):
                    cout[h, :, half * 2 + q, c] = v[q].astype(BF16)

    @pl.loop(0, 2)
    def _(h):
        @pl.loop(0, 4)
        def _(k):
            wait(cin.at[h, 0, pl.ds(0, 7)], r2.at[h, k])

        plane_y(h)

        @pl.loop(0, 2)
        def _(y):
            plane_x(2 * y, 0)
            plane_x(2 * y + 1, 1)
            plane_x_back(2 * y, 0)
            plane_x_back(2 * y + 1, 1)

        plane_y_back(h)

        @pl.loop(0, 4)
        def _(k):
            @pl.loop(1, 8)
            def _(j):
                copy3(h, k, j).start()

        din[h, :, yc] = cout[h, yc]

    def stage_d(h, k):
        zs = (zl + k + 3) % 4
        o = mmt(eye[...], din[h, zs].reshape(128, 256))
        dout[h, zs] = o.astype(BF16).reshape(8, 32, 128)

    @pl.loop(0, 2)
    def _(h):
        @pl.loop(0, 4)
        def _(k):
            wait(din.at[h, 0, pl.ds(0, 7)], r3.at[h, k])
            stage_d(h, k)
            start_all(copy4, h, k, 1)

        ein[h, zl, xh] = dout[h, zl, xh]

    for h in range(2):
        @pl.loop(0, 4)
        def _(k, h=h):
            wait_all(ein, r4, h, k, 1)

        parts = [jnp.concatenate([ein[h, g, s] for s in range(8)], axis=1) for g in range(4)]
        o = mm(jnp.concatenate(parts, axis=0), p3[...]).astype(BF16)
        for g in range(4):
            for x in range(8):
                zb[h, x, :, g * 128:g * 128 + 128] = o[g * 32:g * 32 + 32, x * 128:x * 128 + 128]
        nl = mm(zb[h].reshape(256, 512), last[h * 512:h * 512 + 512, :]) * (1.0 / 32.0)
        base = field if h == 0 else out
        u = base[0].reshape(256, 256) - nl[:, 256:]
        v = base[1].reshape(256, 256) + nl[:, :256]
        out[0] = u.reshape(8, 32, 256)
        out[1] = v.reshape(8, 32, 256)

    shells[...] = shell_sums(u * u + v * v, rad2, reach)
    first[me1] = shells[...]

    @pl.loop(1, 16)
    def _(i):
        copy5(i).start()

    az = PHASE_RATE * (wz * wz).astype(F32)
    ar = PHASE_RATE * rad2.astype(F32)
    cz, sz = jnp.cos(az), jnp.sin(az)
    cr, sr = jnp.cos(ar), jnp.sin(ar)
    cos = (cr * cz - sr * sz).reshape(8, 32, 256)
    sin = (sr * cz + cr * sz).reshape(8, 32, 256)
    u, v = out[0], out[1]
    out[0] = u * cos + v * sin
    out[1] = v * cos - u * sin

    wait(first.at[pl.ds(0, 15)], r5.at[0])

    mid[...] = jnp.sum(first[...], axis=0)
    second[me2] = mid[...]

    @pl.loop(1, 16)
    def _(i):
        copy6(i).start()

    wait(second.at[pl.ds(0, 15)], r6.at[0])

    spectrum[...] = jnp.sum(second[...], axis=0) / counts[...]

    @pl.loop(0, 2)
    def _(h):
        @pl.loop(0, 4)
        def _(k):
            wait_all(aout, s1, h, k, 2)
            wait(bout.at[h, pl.ds(0, 7), 0], s2.at[h, k])
            wait(cout.at[h, pl.ds(0, 7), 0], s3.at[h, k])
            wait_all(dout, s4, h, k, 1)

    wait(first.at[pl.ds(0, 15)], s5.at[0])
    wait(second.at[pl.ds(0, 15)], s6.at[0])


def tables():
    waves = np.arange(K, dtype=np.int64) - K // 2
    phase = (waves[:, None] * np.arange(N, dtype=np.int64)[None, :]) % N
    angle = phase.astype(np.float32) * np.float32(2.0 * math.pi / N)
    cos = np.cos(angle).astype(jnp.bfloat16)
    sin = np.sin(angle).astype(jnp.bfloat16)
    fwd = np.concatenate([cos, sin], axis=0)
    inv = np.concatenate([cos.T, sin.T], axis=1)
    h, g, c, s, z = np.meshgrid(*(np.arange(n) for n in (2, 4, 2, 8, 8)), indexing="ij")
    point = ((g * 8 + s) * 16 + h * 8 + z).reshape(-1)
    is_re = (c.reshape(-1) == 0)[:, None]
    ct, st = cos.T[point], sin.T[point]
    last = np.concatenate([np.where(is_re, ct, st), np.where(is_re, -st, ct)], axis=1)
    sq = waves * waves
    q = (sq[:, None] + sq[None, :]).reshape(-1)
    pairs = np.bincount(q, minlength=2 * (K // 2) ** 2 + 1)
    counts = np.zeros(K, np.float64)
    radii = np.nonzero(pairs)[0]
    for w2 in sq:
        shell = np.floor(np.sqrt((radii + w2).astype(np.float64)) + 0.5).astype(np.int64)
        counts += np.bincount(shell, weights=pairs[radii], minlength=K)[:K]
    return fwd, np.ascontiguousarray(inv), last, np.maximum(counts, 1.0).astype(np.float32).reshape(1, K)


VMEM = pl.BlockSpec(memory_space=pltpu.VMEM)
HBM = pl.BlockSpec(memory_space=pltpu.HBM)


def body(spectral_field, fwd, inv, last, counts):
    updated, spectrum = pl.pallas_call(
        transform_kernel,
        out_shape=(
            pltpu.VMEM((2, 8, 32, 256), F32),
            pltpu.VMEM((1, 256), F32),
        ),
        in_specs=[HBM] * 5,
        out_specs=(VMEM, VMEM),
        scratch_shapes=[
            pltpu.VMEM((2, 8, 32, 256), F32),
            pltpu.VMEM((512, 512), BF16),
            pltpu.VMEM((512, 512), BF16),
            pltpu.VMEM((1024, 512), BF16),
            pltpu.VMEM((1, 256), F32),
            pltpu.VMEM((512, 512), BF16),
            pltpu.VMEM((128, 128), BF16),
            pltpu.VMEM((1024, 1024), BF16),
            pltpu.VMEM((256, 256), BF16),
            pltpu.VMEM((2, 4, 8, 2, 8, 256), BF16),
            pltpu.VMEM((2, 4, 8, 2, 8, 256), BF16),
            pltpu.VMEM((2, 8, 8, 256), BF16),
            pltpu.VMEM((2, 8, 4, 2, 8, 256), BF16),
            pltpu.VMEM((2, 4, 8, 2, 8, 256), BF16),
            pltpu.VMEM((4, 2, 256, 128), BF16),
            pltpu.VMEM((2, 512, 256), BF16),
            pltpu.VMEM((4, 2, 256, 128), BF16),
            pltpu.VMEM((2, 8, 4, 2, 8, 256), BF16),
            pltpu.VMEM((2, 4, 8, 2, 8, 256), BF16),
            pltpu.VMEM((2, 4, 8, 32, 128), BF16),
            pltpu.VMEM((2, 4, 8, 32, 128), BF16),
            pltpu.VMEM((2, 8, 32, 512), BF16),
            pltpu.VMEM((2, 256, 128), jnp.int32),
            pltpu.VMEM((1, 256), F32),
            pltpu.VMEM((16, 1, 256), F32),
            pltpu.VMEM((16, 1, 256), F32),
            pltpu.VMEM((1, 256), F32),
        ] + [pltpu.SemaphoreType.DMA((2, 4))] * 8 + [pltpu.SemaphoreType.DMA((5,))] + [
            pltpu.SemaphoreType.DMA((1,))] * 4,
        compiler_params=pltpu.CompilerParams(
            collective_id=0, has_side_effects=True, vmem_limit_bytes=50 * 1024 * 1024),
        name="transforms",
    )(*(pltpu.with_memory_space_constraint(x, pltpu.HBM) for x in (spectral_field, fwd, inv, last, counts)))
    return updated, spectrum.reshape(256)


def solution(mesh):
    consts = tables()
    step = functools.partial(jax.shard_map, mesh=mesh, check_vma=False)

    def run(spectral_field):
        return step(
            lambda f: body(f, *(jnp.asarray(c) for c in consts)),
            in_specs=(P(None, "row", "col", None),),
            out_specs=(P(None, "row", "col", None), P()),
        )(spectral_field)

    return run
```

```python
import functools
import math

import jax
import jax.numpy as jnp
import numpy as np
from jax import lax
from jax.experimental import pallas as pl
from jax.experimental.pallas import tpu as pltpu
from jax.sharding import PartitionSpec as P

PHASE_RATE = 0.0002
COUPLING = 0.2
K = 256
N = 512
BF16 = jnp.bfloat16
F32 = jnp.float32


def mm(a, b):
    return lax.dot_general(a, b, (((1,), (0,)), ((), ())), preferred_element_type=F32)


def mmt(a, b):
    return lax.dot_general(a, b, (((1,), (1,)), ((), ())), preferred_element_type=F32)


def iota(shape, dim):
    return lax.broadcasted_iota(jnp.int32, shape, dim)


def one_hot(hit):
    return jnp.where(hit, 1.0, 0.0).astype(BF16)


def shell_room(rad2, part):
    s = iota((1, 128), 1) + part * 128
    return s * s + s - rad2


def shell_reach(rad2, part):
    room = jnp.maximum(shell_room(rad2, part), 0).astype(F32)
    return jnp.minimum(jnp.sqrt(room + 0.5).astype(jnp.int32), 127)


def shell_sums(energy, rad2, reach):
    j = jnp.abs(iota((256, 128), 0) - 128)
    within = jnp.where(j <= iota((256, 128), 1), 1.0, 0.0)
    prefix = lax.dot_general(energy, within, (((1,), (0,)), ((), ())),
                             preferred_element_type=F32, precision=lax.Precision.HIGHEST)
    parts = []
    for part in range(2):
        room = shell_room(rad2, part)
        inner = jnp.take_along_axis(prefix, reach[part], axis=1, mode="promise_in_bounds")
        total = jnp.where(room >= 0, inner, 0.0) + jnp.where(room >= 128 * 128, energy[:, :1], 0.0)
        parts.append(jnp.sum(total, axis=0, keepdims=True))
    lane = iota((1, 256), 1)
    shifted = jnp.concatenate([pltpu.roll(parts[0], 1, 1), pltpu.roll(parts[1], 1, 1)], axis=1)
    shifted = jnp.where(lane == 0, 0.0, jnp.where(lane == 128, parts[0][:, 127:], shifted))
    return jnp.concatenate(parts, axis=1) - shifted


def transform_kernel(
    field_hbm, fwd_hbm, inv_hbm, last_hbm, counts_hbm, out, spectrum,
    field, fwd, inv, last, counts, p1, p2, p3, eye, aout, bin_, xr, bout, cin, yb, cub, xb, cout, din, dout, ein, zb, reach,
    shells, first, second, mid,
    s1, r1, s2, r2, s3, r3, s4, r4, load_sem, s5, r5, s6, r6,
):
    row = lax.axis_index("row")
    xh = lax.axis_index("col")
    zl = row // 8
    yc = row % 8

    def remote(src, dst, send, recv, to_row, to_col):
        return pltpu.make_async_remote_copy(
            src_ref=src, dst_ref=dst, send_sem=send, recv_sem=recv,
            device_id={"row": to_row, "col": to_col}, device_id_type=pl.DeviceIdType.MESH,
        )

    loads = [
        pltpu.make_async_copy(field_hbm, field, load_sem.at[0]),
        pltpu.make_async_copy(inv_hbm, inv, load_sem.at[1]),
        pltpu.make_async_copy(fwd_hbm, fwd, load_sem.at[2]),
        pltpu.make_async_copy(last_hbm, last, load_sem.at[3]),
        pltpu.make_async_copy(counts_hbm, counts, load_sem.at[4]),
    ]
    for load in loads[:2]:
        load.start()

    barrier = pltpu.get_barrier_semaphore()

    @pl.loop(1, 32)
    def _(i):
        d = (zl * 8 + xh + i) % 32
        pl.semaphore_signal(
            barrier, inc=1, device_id={"row": (d // 8) * 8 + yc, "col": d % 8},
            device_id_type=pl.DeviceIdType.MESH,
        )

    @pl.loop(1, 8)
    def _(j):
        pl.semaphore_signal(
            barrier, inc=1, device_id={"row": zl * 8 + (yc + j) % 8, "col": xh},
            device_id_type=pl.DeviceIdType.MESH,
        )

    def wait(ref, sem):
        pltpu.make_async_copy(ref, ref, sem).wait()

    def copy1(h, k, i):
        zd = (zl + 6 - k) % 4
        xd = (xh + i) % 8
        return remote(aout.at[h, zd, xd], bin_.at[h, zl, xh], s1.at[h, k], r1.at[h, k], zd * 8 + yc, xd)

    def copy2(h, k, j):
        zs = (zl + k + 2) % 4
        yd = (yc + j) % 8
        return remote(bout.at[h, yd, zs], cin.at[h, zs, yc], s2.at[h, k], r2.at[h, k], zl * 8 + yd, xh)

    def copy3(h, k, j):
        zs = (zl + k + 3) % 4
        yd = (yc + j) % 8
        return remote(cout.at[h, yd, zs], din.at[h, zs, yc], s3.at[h, k], r3.at[h, k], zl * 8 + yd, xh)

    def copy4(h, k, i):
        zd = (zl + k + 3) % 4
        xd = (xh + i) % 8
        return remote(dout.at[h, zd, xd], ein.at[h, zl, xh], s4.at[h, k], r4.at[h, k], zd * 8 + yc, xd)

    def start_all(copy, h, k, own):
        @pl.when(jnp.asarray(k) != own)
        def _():
            copy(h, k, 0).start()

        @pl.loop(1, 8)
        def _(i):
            copy(h, k, i).start()

    def wait_all(ref, sem, h, k, own):
        @pl.when(k != own)
        def _():
            wait(ref.at[h, 0], sem.at[h, k])

        @pl.when(k == own)
        def _():
            wait(ref.at[h, 0, pl.ds(0, 7)], sem.at[h, k])

    xc, z_hi, yy, core = xh // 2, xh % 2, yc // 2, yc % 2
    me1 = xc * 4 + yy
    me2 = (z_hi * 4 + zl) * 2 + core

    def copy5(i):
        d = (me1 + i) % 16
        return remote(shells, first.at[me1], s5.at[0], r5.at[0], zl * 8 + (d % 4) * 2 + core, (d // 4) * 2 + z_hi)

    def copy6(i):
        d = (me2 + i) % 16
        return remote(
            mid, second.at[me2], s6.at[0], r6.at[0], ((d // 2) % 4) * 8 + yy * 2 + d % 2, xc * 2 + d // 8)

    for load in loads[2:]:
        load.start()
    loads[0].wait()
    loads[1].wait()

    def stage_a(k):
        zd = (zl + 6 - k) % 4
        rows = pl.ds(pl.multiple_of(zd * 128, 128), 128)
        c, s = inv[rows, :256], inv[rows, 256:]
        re = field[0].reshape(256, 256).astype(BF16)
        im = field[1].reshape(256, 256).astype(BF16)
        pair = (
            (mmt(c, re) - mmt(s, im)) * (1.0 / 16.0),
            (mmt(s, re) + mmt(c, im)) * (1.0 / 16.0),
        )
        for ri in range(2):
            v = pair[ri].reshape(8, 2, 8, 256)
            for h in range(2):
                aout[h, zd, :, ri] = v[:, h].astype(BF16)

    stage_a(0)
    pl.semaphore_wait(barrier, 38)
    start_all(copy1, 0, 0, 2)

    @pl.loop(1, 4)
    def _(k):
        stage_a(k)
        start_all(copy1, 0, k, 2)

    @pl.loop(0, 4)
    def _(k):
        start_all(copy1, 1, k, 2)

    for h in range(2):
        bin_[h, zl, xh] = aout[h, zl, xh]

    j1 = iota((128, 512), 1)
    f1 = ((j1 // 32) % 4) * 128 + (j1 // 128) * 32 + j1 % 32

    @pl.loop(0, 4)
    def _(b):
        rows = pl.ds(pl.multiple_of(b * 128, 128), 128)
        p1[rows, :] = one_hot(iota((128, 512), 0) + b * 128 == f1)

    q2 = iota((128, 128), 0)
    p2[...] = one_hot(iota((128, 128), 1) == (q2 // 64) * 64 + (q2 % 8) * 8 + (q2 // 8) % 8)

    eye[...] = one_hot(iota((256, 256), 0) == iota((256, 256), 1))
    j3 = iota((128, 1024), 1)
    f3 = ((j3 // 8) % 8) * 128 + (j3 % 8) * 16 + ((j3 // 64) % 2) * 8 + j3 // 128

    @pl.loop(0, 8)
    def _(b):
        rows = pl.ds(pl.multiple_of(b * 128, 128), 128)
        p3[rows, :] = one_hot(iota((128, 1024), 0) + b * 128 == f3)

    wz = iota((1, 256), 1) - 128
    r = iota((256, 1), 0)
    wx = row * 8 - 128 + r // 32
    wy = xh * 32 - 128 + r % 32
    rad2 = wx * wx + wy * wy
    for part in range(2):
        reach[part] = shell_reach(rad2, part)

    loads[2].wait()
    loads[3].wait()
    loads[4].wait()

    def stage_b(h, k):
        zs = (zl + k + 2) % 4
        parts = []
        for ht in range(2):
            for xt in range(2):
                lanes = slice(xt * 128, xt * 128 + 128)
                parts.append(jnp.concatenate(
                    [bin_[h, zs, ht * 4 + q, :, :, lanes].reshape(16, 128) for q in range(4)], axis=1))
        o = mm(jnp.concatenate(parts, axis=0), p1[...])
        for ht in range(2):
            for xt in range(2):
                base = (ht * 2 + xt) * 16
                for c in range(2):
                    for x in range(4):
                        xr[c, xt * 4 + x, :, ht * 128:ht * 128 + 128] = (
                            o[base + c * 8:base + c * 8 + 8, x * 128:x * 128 + 128].astype(BF16))
        q = mm(p2[...], xr[...].reshape(128, 256)).reshape(2, 8, 8, 256)
        for c in range(2):
            bout[h, :, zs, c] = q[c].astype(BF16)
        cin[h, zs, yc] = bout[h, yc, zs]

    @pl.loop(0, 2)
    def _(h):
        @pl.loop(0, 4)
        def _(k):
            wait_all(bin_, r1, h, k, 2)
            stage_b(h, k)

            @pl.loop(1, 8)
            def _(j):
                copy2(h, k, j).start()

    def plane_y(h):
        for half in range(2):
            d = jnp.concatenate(
                [cin[h, half * 2:half * 2 + 2, :, c].reshape(128, 256) for c in range(2)], axis=0)
            mc = mm(d, fwd[:256, :])
            ms = mm(d, fwd[256:, :])
            pair = ((mc[:128] - ms[128:]) * (1.0 / 16.0), (ms[:128] + mc[128:]) * (1.0 / 16.0))
            for c in range(2):
                for y in range(4):
                    yb[y, c, half * 128:half * 128 + 128, :] = pair[c][:, y * 128:y * 128 + 128].astype(BF16)

    def plane_x(y, slot):
        d = jnp.concatenate([yb[y, 0], yb[y, 1]], axis=1)
        d = jnp.concatenate([d, jnp.concatenate([-d[:, 128:], d[:, :128]], axis=1)], axis=0)
        for half in range(2):
            rows = slice(half * 256, half * 256 + 256)
            phys = mm(inv[rows, :], d) * (1.0 / 16.0)
            re, im = phys[:, :128], phys[:, 128:]
            gain = COUPLING * (re * re + im * im)
            cub[slot, rows, :128] = (gain * re).astype(BF16)
            cub[slot, rows, 128:] = (gain * im).astype(BF16)

    def plane_x_back(y, slot):
        m = mm(fwd[...], cub[slot])
        xb[y, 0] = ((m[:256, :128] + m[256:, 128:]) * (1.0 / 32.0)).astype(BF16)
        xb[y, 1] = ((m[:256, 128:] - m[256:, :128]) * (1.0 / 32.0)).astype(BF16)

    def plane_y_back(h):
        for half in range(2):
            rows = slice(half * 128, half * 128 + 128)
            d = jnp.concatenate(
                [jnp.concatenate([xb[y, c, rows, :] for y in range(4)], axis=1) for c in range(2)], axis=0)
            m = mm(d, inv[...])
            pair = (
                (m[:128, :256] + m[128:, 256:]) * (1.0 / 32.0),
                (m[128:, :256] - m[:128, 256:]) * (1.0 / 32.0),
            )
            for c in range(2):
                v = pair[c].reshape(2, 8, 8, 256)
                for q in range(2):
                    cout[h, :, half * 2 + q, c] = v[q].astype(BF16)

    @pl.loop(0, 2)
    def _(h):
        @pl.loop(0, 4)
        def _(k):
            wait(cin.at[h, 0, pl.ds(0, 7)], r2.at[h, k])

        plane_y(h)

        for y in range(2):
            plane_x(2 * y, 0)
            plane_x(2 * y + 1, 1)
            plane_x_back(2 * y, 0)
            plane_x_back(2 * y + 1, 1)

        plane_y_back(h)

        @pl.loop(0, 4)
        def _(k):
            @pl.loop(1, 8)
            def _(j):
                copy3(h, k, j).start()

        din[h, :, yc] = cout[h, yc]

    def stage_d(h, k):
        zs = (zl + k + 3) % 4
        o = mmt(eye[...], din[h, zs].reshape(128, 256))
        dout[h, zs] = o.astype(BF16).reshape(8, 32, 128)

    @pl.loop(0, 2)
    def _(h):
        @pl.loop(0, 4)
        def _(k):
            wait(din.at[h, 0, pl.ds(0, 7)], r3.at[h, k])
            stage_d(h, k)
            start_all(copy4, h, k, 1)

        ein[h, zl, xh] = dout[h, zl, xh]

    for h in range(2):
        @pl.loop(0, 4)
        def _(k, h=h):
            wait_all(ein, r4, h, k, 1)

        parts = [jnp.concatenate([ein[h, g, s] for s in range(8)], axis=1) for g in range(4)]
        o = mm(jnp.concatenate(parts, axis=0), p3[...]).astype(BF16)
        for g in range(4):
            for x in range(8):
                zb[h, x, :, g * 128:g * 128 + 128] = o[g * 32:g * 32 + 32, x * 128:x * 128 + 128]
        nl = mm(zb[h].reshape(256, 512), last[h * 512:h * 512 + 512, :]) * (1.0 / 32.0)
        base = field if h == 0 else out
        u = base[0].reshape(256, 256) - nl[:, 256:]
        v = base[1].reshape(256, 256) + nl[:, :256]
        out[0] = u.reshape(8, 32, 256)
        out[1] = v.reshape(8, 32, 256)

    shells[...] = shell_sums(u * u + v * v, rad2, reach)
    first[me1] = shells[...]

    @pl.loop(1, 16)
    def _(i):
        copy5(i).start()

    az = PHASE_RATE * (wz * wz).astype(F32)
    ar = PHASE_RATE * rad2.astype(F32)
    cz, sz = jnp.cos(az), jnp.sin(az)
    cr, sr = jnp.cos(ar), jnp.sin(ar)
    cos = (cr * cz - sr * sz).reshape(8, 32, 256)
    sin = (sr * cz + cr * sz).reshape(8, 32, 256)
    u, v = out[0], out[1]
    out[0] = u * cos + v * sin
    out[1] = v * cos - u * sin

    wait(first.at[pl.ds(0, 15)], r5.at[0])

    mid[...] = jnp.sum(first[...], axis=0)
    second[me2] = mid[...]

    @pl.loop(1, 16)
    def _(i):
        copy6(i).start()

    wait(second.at[pl.ds(0, 15)], r6.at[0])

    spectrum[...] = jnp.sum(second[...], axis=0) / counts[...]

    @pl.loop(0, 2)
    def _(h):
        @pl.loop(0, 4)
        def _(k):
            wait_all(aout, s1, h, k, 2)
            wait(bout.at[h, pl.ds(0, 7), 0], s2.at[h, k])
            wait(cout.at[h, pl.ds(0, 7), 0], s3.at[h, k])
            wait_all(dout, s4, h, k, 1)

    wait(first.at[pl.ds(0, 15)], s5.at[0])
    wait(second.at[pl.ds(0, 15)], s6.at[0])


def tables():
    waves = np.arange(K, dtype=np.int64) - K // 2
    phase = (waves[:, None] * np.arange(N, dtype=np.int64)[None, :]) % N
    angle = phase.astype(np.float32) * np.float32(2.0 * math.pi / N)
    cos = np.cos(angle).astype(jnp.bfloat16)
    sin = np.sin(angle).astype(jnp.bfloat16)
    fwd = np.concatenate([cos, sin], axis=0)
    inv = np.concatenate([cos.T, sin.T], axis=1)
    h, g, c, s, z = np.meshgrid(*(np.arange(n) for n in (2, 4, 2, 8, 8)), indexing="ij")
    point = ((g * 8 + s) * 16 + h * 8 + z).reshape(-1)
    is_re = (c.reshape(-1) == 0)[:, None]
    ct, st = cos.T[point], sin.T[point]
    last = np.concatenate([np.where(is_re, ct, st), np.where(is_re, -st, ct)], axis=1)
    sq = waves * waves
    q = (sq[:, None] + sq[None, :]).reshape(-1)
    pairs = np.bincount(q, minlength=2 * (K // 2) ** 2 + 1)
    counts = np.zeros(K, np.float64)
    radii = np.nonzero(pairs)[0]
    for w2 in sq:
        shell = np.floor(np.sqrt((radii + w2).astype(np.float64)) + 0.5).astype(np.int64)
        counts += np.bincount(shell, weights=pairs[radii], minlength=K)[:K]
    return fwd, np.ascontiguousarray(inv), last, np.maximum(counts, 1.0).astype(np.float32).reshape(1, K)


VMEM = pl.BlockSpec(memory_space=pltpu.VMEM)
HBM = pl.BlockSpec(memory_space=pltpu.HBM)


def body(spectral_field, fwd, inv, last, counts):
    updated, spectrum = pl.pallas_call(
        transform_kernel,
        out_shape=(
            pltpu.VMEM((2, 8, 32, 256), F32),
            pltpu.VMEM((1, 256), F32),
        ),
        in_specs=[HBM] * 5,
        out_specs=(VMEM, VMEM),
        scratch_shapes=[
            pltpu.VMEM((2, 8, 32, 256), F32),
            pltpu.VMEM((512, 512), BF16),
            pltpu.VMEM((512, 512), BF16),
            pltpu.VMEM((1024, 512), BF16),
            pltpu.VMEM((1, 256), F32),
            pltpu.VMEM((512, 512), BF16),
            pltpu.VMEM((128, 128), BF16),
            pltpu.VMEM((1024, 1024), BF16),
            pltpu.VMEM((256, 256), BF16),
            pltpu.VMEM((2, 4, 8, 2, 8, 256), BF16),
            pltpu.VMEM((2, 4, 8, 2, 8, 256), BF16),
            pltpu.VMEM((2, 8, 8, 256), BF16),
            pltpu.VMEM((2, 8, 4, 2, 8, 256), BF16),
            pltpu.VMEM((2, 4, 8, 2, 8, 256), BF16),
            pltpu.VMEM((4, 2, 256, 128), BF16),
            pltpu.VMEM((2, 512, 256), BF16),
            pltpu.VMEM((4, 2, 256, 128), BF16),
            pltpu.VMEM((2, 8, 4, 2, 8, 256), BF16),
            pltpu.VMEM((2, 4, 8, 2, 8, 256), BF16),
            pltpu.VMEM((2, 4, 8, 32, 128), BF16),
            pltpu.VMEM((2, 4, 8, 32, 128), BF16),
            pltpu.VMEM((2, 8, 32, 512), BF16),
            pltpu.VMEM((2, 256, 128), jnp.int32),
            pltpu.VMEM((1, 256), F32),
            pltpu.VMEM((16, 1, 256), F32),
            pltpu.VMEM((16, 1, 256), F32),
            pltpu.VMEM((1, 256), F32),
        ] + [pltpu.SemaphoreType.DMA((2, 4))] * 8 + [pltpu.SemaphoreType.DMA((5,))] + [
            pltpu.SemaphoreType.DMA((1,))] * 4,
        compiler_params=pltpu.CompilerParams(
            collective_id=0, has_side_effects=True, vmem_limit_bytes=50 * 1024 * 1024),
        name="transforms",
    )(*(pltpu.with_memory_space_constraint(x, pltpu.HBM) for x in (spectral_field, fwd, inv, last, counts)))
    return updated, spectrum.reshape(256)


def solution(mesh):
    consts = tables()
    step = functools.partial(jax.shard_map, mesh=mesh, check_vma=False)

    def run(spectral_field):
        return step(
            lambda f: body(f, *(jnp.asarray(c) for c in consts)),
            in_specs=(P(None, "row", "col", None),),
            out_specs=(P(None, "row", "col", None), P()),
        )(spectral_field)

    return run
```
